32 devices in a mesh: gx: 8 (over y, x, core), gy: 4 (over z).
Axes of the slice: x: 2, y: 2, z: 4, core: 2. Of those that a mesh axis runs over, the one named last changes fastest.
Arguments:
- source: float32 [160, 80, 640], P('gx', 'gy'), may hold values from -210 to 210
- conductivity: float32 [160, 80, 640], P('gx', 'gy'), may hold values from 0.001 to 1
- absorption: float32 [160, 80, 640], P('gx', 'gy'), may hold values from 1 to 10
Outputs:
- solution: float32 [160, 80, 640], P('gx', 'gy')
- correction: float32 [96, 48, 384], P('gx', 'gy')
The draws below stay inside these ranges and needn't reach their ends.
All inputs are finite; a program needn't handle non-finite values.
Results may differ from the reference program's by a relative error of at most 0.00023.
Values sent between devices are 32-bit elements; how exact they have to be, the bound alone decides.
A program may use at most 128 MiB of HBM per device.

```python
import math
import jax
import jax.numpy as jnp
import numpy as np
from jax import lax

SWEEPS = 3
NX = 160
NY = 80
NZ = 640


def draw_source(key, part):
    first = jax.random.fold_in(key, 0)
    shape = (NX, NY, NZ)
    rise_x = 3.0 ** (jnp.arange(NX, dtype=jnp.float32) / NX)
    rise_y = 3.0 ** (jnp.arange(NY, dtype=jnp.float32) / NY)
    ramp = rise_x[:, None, None] * rise_y[None, :, None]
    base = jax.random.truncated_normal(first, -4.0, 4.0, shape, jnp.float32)
    return (base * ramp).astype(jnp.float32)


def draw_conductivity(key, part):
    inner = jax.random.fold_in(key, 17)
    shape = (NX, NY, NZ)
    place_x = jnp.arange(NX, dtype=jnp.float32) / NX
    place_y = jnp.arange(NY, dtype=jnp.float32) / NY
    rise_x = 10.0 ** place_x / 10.0
    base = jnp.exp(jax.random.uniform(inner, shape, jnp.float32, math.log(0.1), 0.0))
    rise_y = 3.0 ** place_y / 3.0
    ramp = rise_x[:, None, None] * rise_y[None, :, None]
    return (base * ramp).astype(jnp.float32)


def levels(stream_key, dims, cuts, low, largest):
    gain, own = 1.0, jax.random.fold_in(stream_key, 6)
    for position, blocks in cuts:
        steps = jnp.exp(jax.random.uniform(jax.random.fold_in(own, position), (blocks,), jnp.float32, low / len(cuts), largest / len(cuts)))
        gain = gain * jnp.repeat(steps, dims[position] // blocks).reshape([-1 if axis == position else 1 for axis in range(len(dims))])
    return gain


def setup_inputs(seed: int = 0) -> dict:
    splits = jax.random.split(jax.random.key(seed), 4)
    return {
        "source": draw_source(jax.random.fold_in(splits[3], 71), 0),
        "conductivity": draw_conductivity(jax.random.fold_in(splits[3], 71), 0),
        "absorption": jnp.clip(jnp.exp(math.log(10.0) - 2.3025851 * jax.random.uniform(splits[2], (NX, NY, NZ), jnp.float32) ** levels(splits[2], (NX, NY, NZ), ((0, 8), (1, 4)), -0.2, 0.2)), 1.0, 10.0),
    }


HIGH = lax.Precision.HIGHEST

def deriv_table(points):
    count = len(points)
    barycentric = np.array([1.0 / np.prod([points[j] - points[k] for k in range(count) if k != j]) for j in range(count)])
    table = np.zeros((count, count))
    for i in range(count):
        for j in range(count):
            if i != j:
                table[i, j] = barycentric[j] / (barycentric[i] * (points[i] - points[j]))
        table[i, i] = -np.sum(table[i])
    return table

def make_tables():
    root = math.sqrt(3.0 / 7.0)
    fine_points = np.array([-1.0, -root, 0.0, root, 1.0])
    fine_weights = np.array([0.1, 49.0 / 90.0, 32.0 / 45.0, 49.0 / 90.0, 0.1])
    coarse_points = np.array([-1.0, 0.0, 1.0])
    coarse_weights = np.array([1.0 / 3.0, 4.0 / 3.0, 1.0 / 3.0])
    interp = np.stack([fine_points * (fine_points - 1.0) / 2.0, 1.0 - fine_points ** 2, fine_points * (fine_points + 1.0) / 2.0], 1)
    select = np.zeros((3, 5))
    select[0, 0] = 1.0
    select[1, 2] = 1.0
    select[2, 4] = 1.0
    return [jnp.asarray(t, jnp.float32) for t in (fine_weights, coarse_weights, deriv_table(fine_points), deriv_table(coarse_points), interp, select)]

def along(field, table, axis):
    count_out, count_in = table.shape
    shape = field.shape
    elems = shape[axis] // count_in
    split = field.reshape(shape[:axis] + (elems, count_in) + shape[axis + 1:])
    moved = jnp.moveaxis(split, axis + 1, -1)
    mixed = jnp.einsum('...i,pi->...p', moved, table, precision=HIGH)
    back = jnp.moveaxis(mixed, -1, axis + 1)
    return back.reshape(shape[:axis] + (elems * count_out,) + shape[axis + 1:])

def end_masks(length, count, axis):
    index = jnp.arange(length) % count
    shape = [1, 1, 1]
    shape[axis] = length
    return ((index == 0).reshape(shape), (index == count - 1).reshape(shape))

def assemble(field, count):
    for axis in range(3):
        lower, upper = end_masks(field.shape[axis], count, axis)
        field = field + jnp.where(upper, jnp.roll(field, -1, axis), 0.0) + jnp.where(lower, jnp.roll(field, 1, axis), 0.0)
    return field

def node_weights(shape, weights):
    count = weights.shape[0]
    first = jnp.tile(weights, shape[0] // count)
    second = jnp.tile(weights, shape[1] // count)
    third = jnp.tile(weights, shape[2] // count)
    return first[:, None, None] * second[None, :, None] * third[None, None, :]

def half_ends(shape, count):
    parts = []
    for axis in range(3):
        lower, upper = end_masks(shape[axis], count, axis)
        parts.append(jnp.where(lower | upper, 0.5, 1.0))
    return parts[0] * parts[1] * parts[2]

def local_op(field, flux, mass, deriv):
    result = mass * field
    for axis in range(3):
        result = result + along(flux * along(field, deriv, axis), deriv.T, axis)
    return result

def local_diag(flux, mass, deriv):
    result = mass
    square = (deriv * deriv).T
    for axis in range(3):
        result = result + along(flux, square, axis)
    return result

def chebyshev(rhs, apply, inverse, estimate, want_residual):
    theta = 0.75 * estimate
    delta = 0.45 * estimate
    sigma = 5.0 / 3.0
    rho = 0.6
    solution = jnp.zeros_like(rhs)
    residual = rhs
    direction = inverse * residual / theta
    for sweep in range(SWEEPS):
        solution = solution + direction
        if sweep + 1 < SWEEPS or want_residual:
            residual = residual - apply(direction)
        if sweep + 1 < SWEEPS:
            rho_next = 1.0 / (2.0 * sigma - rho)
            direction = rho_next * rho * direction + 2.0 * rho_next / delta * inverse * residual
            rho = rho_next
    return (solution, residual)

def estimate_of(start, apply, inverse):
    first = inverse * apply(start)
    second = inverse * apply(first)
    return jnp.sqrt(jnp.sum(second * second) / (jnp.sum(first * first) + 1e-06))

def reference(source, conductivity, absorption):
    fine_weights, coarse_weights, fine_deriv, coarse_deriv, interp, select = make_tables()
    fine_w = node_weights(source.shape, fine_weights)
    fine_flux = fine_w * conductivity
    fine_mass = fine_w * absorption

    def apply_fine(field):
        return assemble(local_op(field, fine_flux, fine_mass, fine_deriv), 5)
    load = assemble(fine_w * source, 5)
    fine_inverse = 1.0 / assemble(local_diag(fine_flux, fine_mass, fine_deriv), 5)
    fine_estimate = estimate_of(load, apply_fine, fine_inverse)
    smoothed, fine_residual = chebyshev(load, apply_fine, fine_inverse, fine_estimate, True)
    coarse_cond = conductivity
    coarse_abs = absorption
    for axis in range(3):
        coarse_cond = along(coarse_cond, select, axis)
        coarse_abs = along(coarse_abs, select, axis)
    coarse_w = node_weights(coarse_cond.shape, coarse_weights)
    coarse_flux = coarse_w * coarse_cond
    coarse_mass = coarse_w * coarse_abs
    halves = half_ends(source.shape, 5)

    def apply_coarse(field):
        return assemble(local_op(field, coarse_flux, coarse_mass, coarse_deriv), 3)

    def restrict(field):
        field = field * halves
        for axis in range(3):
            field = along(field, interp.T, axis)
        return assemble(field, 3)
    coarse_inverse = 1.0 / assemble(local_diag(coarse_flux, coarse_mass, coarse_deriv), 3)
    coarse_estimate = estimate_of(restrict(load), apply_coarse, coarse_inverse)
    correction, unused = chebyshev(restrict(fine_residual), apply_coarse, coarse_inverse, coarse_estimate, False)
    lifted = correction
    for axis in range(3):
        lifted = along(lifted, interp, axis)
    return (smoothed + lifted, correction)
```

```python
import functools
import math

import jax
import jax.numpy as jnp
import numpy as np
from jax import lax
from jax.experimental import pallas as pl
from jax.experimental.pallas import tpu as pltpu
from jax.sharding import PartitionSpec as P

SWEEPS = 3
MESH = pl.DeviceIdType.MESH
DIRS = [(-1, -1), (-1, 1), (1, -1), (1, 1), (0, -1), (0, 1), (-1, 0), (1, 0)]
FINE_STAGES, COARSE_STAGES = 6, 6


def deriv_table(points):
    count = len(points)
    barycentric = np.array(
        [
            1.0 / np.prod([points[j] - points[k] for k in range(count) if k != j])
            for j in range(count)
        ]
    )
    table = np.zeros((count, count))
    for i in range(count):
        for j in range(count):
            if i != j:
                table[i, j] = barycentric[j] / (barycentric[i] * (points[i] - points[j]))
        table[i, i] = -np.sum(table[i])
    return table


ROOT = math.sqrt(3.0 / 7.0)
FINE_POINTS = np.array([-1.0, -ROOT, 0.0, ROOT, 1.0])
FINE_W = np.array([0.1, 49.0 / 90.0, 32.0 / 45.0, 49.0 / 90.0, 0.1])
COARSE_POINTS = np.array([-1.0, 0.0, 1.0])
COARSE_W = np.array([1.0 / 3.0, 4.0 / 3.0, 1.0 / 3.0])
FINE_D = deriv_table(FINE_POINTS)
COARSE_D = deriv_table(COARSE_POINTS)
INTERP = np.stack(
    [
        FINE_POINTS * (FINE_POINTS - 1.0) / 2.0,
        1.0 - FINE_POINTS**2,
        FINE_POINTS * (FINE_POINTS + 1.0) / 2.0,
    ],
    1,
)
RESTRICT = INTERP.T * np.array([0.5, 1.0, 1.0, 1.0, 0.5])[None, :]
TRANSFER = INTERP.T
QF, QC = 5, 3


def chebyshev_coefficients():
    theta, delta, sigma, rho = 0.75, 0.45, 5.0 / 3.0, 0.6
    x = np.zeros(SWEEPS + 1)
    r = np.zeros(SWEEPS + 1)
    r[0] = 1.0
    d = r / theta
    for sweep in range(SWEEPS):
        x = x + d
        r = r - np.concatenate([[0.0], d[:-1]])
        if sweep + 1 < SWEEPS:
            rho_next = 1.0 / (2.0 * sigma - rho)
            d = rho_next * rho * d + 2.0 * rho_next / delta * r
            rho = rho_next
    return [float(v) for v in x[:SWEEPS]]


CHEB = chebyshev_coefficients()


def antisym(table, u):
    n = len(u)
    half = n // 2
    even = [u[j] + u[n - 1 - j] for j in range(half)]
    odd = [u[j] - u[n - 1 - j] for j in range(half)]
    out = [None] * n
    for i in range(half):
        p = float(table[i, half]) * u[half]
        q = None
        for j in range(half):
            s = (table[i, j] + table[i, n - 1 - j]) / 2
            t = (table[i, j] - table[i, n - 1 - j]) / 2
            p = p + float(s) * even[j]
            q = float(t) * odd[j] if q is None else q + float(t) * odd[j]
        out[i] = q + p
        out[n - 1 - i] = q - p
    mid = None
    for j in range(half):
        term = float(table[half, j]) * odd[j]
        mid = term if mid is None else mid + term
    out[half] = mid
    return out


def dense(table, u):
    out = []
    for i in range(table.shape[0]):
        acc = None
        for j in range(table.shape[1]):
            c = float(table[i, j])
            if abs(c) < 1e-14:
                continue
            term = u[j] if c == 1.0 else c * u[j]
            acc = term if acc is None else acc + term
        out.append(acc)
    return out


def plane_starts(q, axis, a, b):
    strides = (q * q, q, 1)
    other = [s for k, s in enumerate(strides) if k != axis]
    return a * other[0] + b * other[1], strides[axis]


def z_sum(line, lanes):
    lo, hi = line[0], line[-1]
    line[-1] = hi + pltpu.roll(lo, lanes - 1, 1)
    line[0] = lo + pltpu.roll(hi, 1, 1)
    return line


def local_op(src, dst, flux, mass, table, lanes):
    q = table.shape[0]

    def lines(axis, a):
        def read(b):
            start, step = plane_starts(q, axis, a, b)
            u = [src[start + step * i] for i in range(q)]
            base = None if axis == 0 else [dst[start + step * i] for i in range(q)]
            return u, base

        ahead = read(0)
        for b in range(q):
            u, base = ahead
            if b + 1 < q:
                ahead = read(b + 1)
            start, step = plane_starts(q, axis, a, b)
            g = antisym(table, u)
            g = [flux[start + step * i] * g[i] for i in range(q)]
            r = antisym(table.T, g)
            for i in range(q):
                r[i] = (mass[start + step * i] * u[i] if base is None else base[i]) + r[i]
            if axis == 2:
                r = z_sum(r, lanes)
            for i in range(q):
                dst[start + step * i] = r[i]

    for axis in range(2):

        @pl.loop(0, q)
        def _(a, axis=axis):
            lines(axis, a)

    for a in range(q):
        lines(2, a)


def local_diag(dst, flux, mass, table, lanes):
    q = table.shape[0]
    square = (table * table).T

    def lines(axis, a):
        for b in range(q):
            start, step = plane_starts(q, axis, a, b)
            r = dense(square, [flux[start + step * i] for i in range(q)])
            for i in range(q):
                base = mass if axis == 0 else dst
                r[i] = base[start + step * i] + r[i]
            if axis == 2:
                r = z_sum(r, lanes)
            for i in range(q):
                dst[start + step * i] = r[i]

    for axis in range(2):

        @pl.loop(0, q)
        def _(a, axis=axis):
            lines(axis, a)

    for a in range(q):
        lines(2, a)


class Lanes:
    def __init__(self, q, rows, ez):
        self.q, self.rows, self.ez = q, rows, ez
        lane = lax.broadcasted_iota(jnp.int32, (rows, ez), 1)
        self.turn = ez % q
        self.back = pow(self.turn, -1, q)
        unit = pow(q, -1, ez)
        self.pick = [lax.rem(lane * q + k, ez) for k in range(q)]
        self.place = [lax.rem((lane + (ez - k)) * unit, ez) for k in range(q)]
        s = lax.rem(lane, q)
        self.out_steps = self.bits(lax.rem(s * (q - self.back), q))
        self.in_steps = self.bits(lax.rem(s * self.back, q))

    def bits(self, amount):
        steps, step = [], 1
        while step < self.q:
            steps.append((step, lax.rem(lax.div(amount, step), 2) == 1))
            step *= 2
        return steps

    def select(self, blocks, steps):
        for step, mask in steps:
            blocks = [
                jnp.where(mask, blocks[(v + step) % self.q], blocks[v]) for v in range(self.q)
            ]
        return blocks

    def split(self, blocks):
        mixed = self.select(blocks, self.out_steps)
        return [
            jnp.take_along_axis(mixed[self.back * k % self.q], self.pick[k], axis=1)
            for k in range(self.q)
        ]

    def merge(self, planes):
        mixed = []
        for j in range(self.q):
            k = self.turn * j % self.q
            mixed.append(jnp.take_along_axis(planes[k], self.place[k], axis=1))
        return self.select(mixed, self.in_steps)


def kernel(
    nx,
    ny,
    src_hbm,
    cond_hbm,
    abs_hbm,
    out_hbm,
    cor_hbm,
    stored,
    result,
    cresult,
    load,
    inv,
    power,
    power_2,
    b0,
    b1,
    b2,
    flux,
    mass,
    smooth,
    coarse,
    tmp_a,
    tmp_b,
    fine_send,
    fine_recv,
    coarse_send,
    coarse_recv,
    line_x_send,
    line_x,
    line_y_send,
    line_y,
    in_sem,
    out_sem,
    cor_sem,
    fine_sems,
    coarse_sems,
    line_send_sem,
    line_x_sem,
    line_y_sem,
):
    px, py, pz = src_hbm.shape
    ex, ey, ez = px // QF, py // QF, pz // QF
    subs, lanes = ex * ey, ez
    tile = 8
    mx, my = lax.axis_index("gx"), lax.axis_index("gy")

    def target(dx, dy):
        return (lax.rem(mx + dx + nx, nx), lax.rem(my + dy + ny, ny))

    greeted = {(o, 0) for o in range(1, nx)} | {(0, o) for o in range(1, ny)}
    greeted |= {(dx % nx, dy % ny) for dx, dy in DIRS}
    greeted = sorted(greeted)
    barrier = pltpu.get_barrier_semaphore()
    for dx, dy in greeted:
        pl.semaphore_signal(barrier, inc=1, device_id=target(dx, dy), device_id_type=MESH)

    arriving = []
    for n, ref in enumerate((src_hbm, cond_hbm, abs_hbm)):
        for v in range(QF):
            copy = pltpu.make_async_copy(
                ref.at[:, :, v * ez : (v + 1) * ez], stored.at[n, v], in_sem.at[n, v]
            )
            copy.start()
            arriving.append(copy)

    sub = lax.broadcasted_iota(jnp.int32, (subs, lanes), 0)
    row_y = lax.rem(sub, ey)
    first_x, last_x = sub < ey, sub >= (ex - 1) * ey
    first_y, last_y = row_y == 0, row_y == ey - 1

    def shifted(plane, shift):
        return pltpu.roll(plane, shift % subs, 0)

    def local_sum(ref, q, zs):
        last = q - 1
        for z in zs:
            for y in range(q):
                p, r = y * q + z, (last * q + y) * q + z
                lo, hi = ref[p], ref[r]
                ref[p] = jnp.where(first_x, lo, lo + shifted(hi, ey))
                ref[r] = jnp.where(last_x, hi, hi + shifted(lo, -ey))
            for x in range(q):
                p, r = x * q * q + z, (x * q + last) * q + z
                lo, hi = ref[p], ref[r]
                ref[p] = jnp.where(first_y, lo, lo + shifted(hi, 1))
                ref[r] = jnp.where(last_y, hi, hi + shifted(lo, -1))

    def edge(dx, dy, q):
        xs = range(q) if dx == 0 else [0 if dx < 0 else q - 1]
        ys = range(q) if dy == 0 else [0 if dy < 0 else q - 1]
        planes = [(x * q + y) * q + z for x in xs for y in ys for z in range(q - 1)]
        e, f = (0 if dx < 0 else ex - 1), (0 if dy < 0 else ey - 1)
        if dy == 0:
            return planes, ey, slice(e * ey, (e + 1) * ey)
        if dx == 0:
            return planes, ex, pl.ds(f, ex, stride=ey)
        return planes, 1, slice(e * ey + f, e * ey + f + 1)

    def whole_rows(count):
        return -(-count // tile) * tile

    pending = []

    def start_exchange(level, stage, fields):
        send, recv, sems = level
        copies = []
        for d, (dx, dy) in enumerate(DIRS):
            at = 0
            for ref, q in fields:
                planes, count, rows = edge(dx, dy, q)
                for p in planes:
                    send[stage, d, at : at + count, :] = ref[p, rows, :]
                    at += count
            total = whole_rows(at)
            copy = pltpu.make_async_remote_copy(
                src_ref=send.at[stage, d, pl.ds(0, total)],
                dst_ref=recv.at[stage, d, pl.ds(0, total)],
                send_sem=sems.at[0, stage, d],
                recv_sem=sems.at[1, stage, d],
                device_id=target(dx, dy),
                device_id_type=MESH,
            )
            copy.start()
            copies.append(copy)
        return copies

    def finish_exchange(level, stage, fields, copies, finals):
        _, recv, _ = level
        for d in reversed(range(len(DIRS))):
            dx, dy = DIRS[d]
            copies[d].wait_recv()
            at = 0
            for ref, q in fields:
                planes, count, rows = edge(-dx, -dy, q)
                for p in planes:
                    ref[p, rows, :] = ref[p, rows, :] + recv[stage, d, at : at + count, :]
                    at += count
        pending.extend(copies)
        for (ref, q), final in zip(fields, finals):
            for x in range(q):
                for y in range(q):
                    if x in (0, q - 1) or y in (0, q - 1):
                        p = (x * q + y) * q
                        for z in range(q - 1):
                            value = final(p + z, ref[p + z])
                            ref[p + z] = value
                            if z == 0:
                                ref[p + q - 1] = pltpu.roll(value, lanes - 1, 1)

    def interior(ref, q, final):
        for x in range(1, q - 1):
            for y in range(1, q - 1):
                for z in range(q):
                    p = (x * q + y) * q + z
                    ref[p] = final(p, ref[p])

    fine = (fine_send, fine_recv, fine_sems)
    rough = (coarse_send, coarse_recv, coarse_sems)

    def start_line(which, along_x, first, second):
        out, slots, sems = (
            (line_x_send, line_x, line_x_sem) if along_x else (line_y_send, line_y, line_y_sem)
        )
        count = nx if along_x else ny
        out[which, 0:1] = first
        out[which, 1:2] = second
        copies = []
        for o in range(1, count):
            copy = pltpu.make_async_remote_copy(
                src_ref=out.at[which],
                dst_ref=slots.at[which, o],
                send_sem=line_send_sem.at[which, 0 if along_x else 1, o],
                recv_sem=sems.at[which, o],
                device_id=target(o, 0) if along_x else target(0, o),
                device_id_type=MESH,
            )
            copy.start()
            copies.append(copy)
        return copies

    def finish_line(which, along_x, copies):
        out, slots = (line_x_send, line_x) if along_x else (line_y_send, line_y)
        count = nx if along_x else ny
        for copy in copies:
            copy.wait_recv()
        pending.extend(copies)
        total = out[which]
        for o in range(1, count):
            total = total + slots[which, o]
        return total[0:1], total[1:2]

    def inverse_estimate(first, second):
        first = jnp.sum(first, axis=1, keepdims=True)
        second = jnp.sum(second, axis=1, keepdims=True)
        return 1.0 / jnp.sqrt(second / (first + 1e-06))

    def coefficients(inv_est):
        power = inv_est
        out = []
        for c in CHEB:
            out.append(jnp.broadcast_to(c * power, (subs, lanes)))
            power = power * inv_est
        return out

    net = Lanes(QF, tile, ez)
    group = tile // ey

    def read_planes(n, x, y):
        tiles = []
        for h in range(subs // tile):
            blocks = []
            for v in range(QF):
                parts = [
                    stored[n, v, (h * group + e) * QF + x, pl.ds(y, ey, stride=QF), :]
                    for e in range(group)
                ]
                blocks.append(jnp.concatenate(parts, axis=0))
            tiles.append(net.split(blocks))
        return tiles

    (
        cflux,
        cmass,
        cinv,
        rload,
        cpow,
        cpow_2,
        rw0,
        rw1,
        rw2,
        crhs,
        cb,
        cw0,
        cw1,
        ccor,
    ) = [coarse.at[i] for i in range(14)]

    for copy in arriving[:QF]:
        copy.wait()
    for x in range(QF):
        for y in range(QF):
            weight = [float(FINE_W[x] * FINE_W[y] * w) for w in FINE_W]
            for h, values in enumerate(read_planes(0, x, y)):
                line = z_sum([w * v for w, v in zip(weight, values)], lanes)
                for z in range(QF):
                    load[(x * QF + y) * QF + z, h * tile : (h + 1) * tile, :] = line[z]
    local_sum(load, QF, range(QF - 1))

    def each(q, body):
        @pl.loop(0, q * q)
        def _(a):
            for i in range(q):
                body(a * q + i)

    def squares(q, values):
        def body(a, acc):
            for i in range(q):
                v = values(a * q + i)
                acc = acc + v * v
            return acc

        total = lax.fori_loop(0, q * q, body, jnp.zeros((subs, lanes), jnp.float32))
        return jnp.sum(total, axis=0, keepdims=True)

    def store(dst, values):
        def body(p):
            dst[p] = values(p)

        return body

    def half_unless(mask):
        return jnp.where(mask, 1.0, 0.5)

    def weighted(line, ends):
        if ends is None:
            return line
        return [half_unless(ends[0]) * line[0]] + line[1:-1] + [half_unless(ends[1]) * line[-1]]

    def restrict(field, dst, summed):
        ends_x = (first_x, last_x) if summed else None
        ends_y = (first_y, last_y) if summed else None

        @pl.loop(0, QF)
        def _(a):
            for c in range(QF):
                line = [field[i * QF * QF + a * QF + c] for i in range(QF)]
                line = dense(TRANSFER, weighted(line, ends_x))
                for i in range(QC):
                    tmp_a[i * QF * QF + a * QF + c] = line[i]

        for a in range(QC):
            for c in range(QF):
                line = [tmp_a[a * QF * QF + i * QF + c] for i in range(QF)]
                line = dense(TRANSFER, weighted(line, ends_y))
                for i in range(QC):
                    tmp_b[a * QC * QF + i * QF + c] = line[i]

        for a in range(QC):
            for c in range(QC):
                line = dense(RESTRICT, [tmp_b[a * QC * QF + c * QF + i] for i in range(QF)])
                line = z_sum(line, lanes)
                for i in range(QC):
                    dst[a * QC * QC + c * QC + i] = line[i]

    def apply_fine(src, dst):
        local_op(src, dst, flux, mass, FINE_D, lanes)

    def apply_coarse(src, dst):
        local_op(src, dst, cflux, cmass, COARSE_D, lanes)

    keep = lambda p, v: v
    invert = lambda p, v: 1.0 / v
    scaled = lambda p, v: inv[p] * v
    cscaled = lambda p, v: cinv[p] * v
    inner_f, inner_c = range(QF - 1), range(QC - 1)

    pl.semaphore_wait(barrier, len(greeted))
    f_load = start_exchange(fine, 0, [(load, QF)])

    pick = {0: 0, 2: 1, 4: 2}
    for n, full, part in ((1, flux, cflux), (2, mass, cmass)):
        for copy in arriving[n * QF : (n + 1) * QF]:
            copy.wait()
        for x in range(QF):
            for y in range(QF):
                for h, values in enumerate(read_planes(n, x, y)):
                    place = slice(h * tile, (h + 1) * tile)
                    for z in range(QF):
                        weight = float(FINE_W[x] * FINE_W[y] * FINE_W[z])
                        full[(x * QF + y) * QF + z, place, :] = weight * values[z]
                        if x in pick and y in pick and z in pick:
                            i, j, k = pick[x], pick[y], pick[z]
                            weight = float(COARSE_W[i] * COARSE_W[j] * COARSE_W[k])
                            part[(i * QC + j) * QC + k, place, :] = weight * values[z]

    local_diag(inv, flux, mass, FINE_D, lanes)
    local_sum(inv, QF, inner_f)
    f_diag = start_exchange(fine, 1, [(inv, QF)])

    local_sum(load, QF, [QF - 1])
    restrict(load, rload, True)
    local_sum(rload, QC, inner_c)
    local_diag(cinv, cflux, cmass, COARSE_D, lanes)
    local_sum(cinv, QC, inner_c)
    c_0 = start_exchange(rough, 0, [(cinv, QC), (rload, QC)])
    interior(inv, QF, invert)

    finish_exchange(fine, 0, [(load, QF)], f_load, [keep])
    apply_fine(load, power)
    local_sum(power, QF, inner_f)
    f_power = start_exchange(fine, 2, [(power, QF)])
    interior(power, QF, scaled)

    finish_exchange(fine, 1, [(inv, QF)], f_diag, [invert])
    each(QF, store(b0, lambda p: inv[p] * load[p]))
    apply_fine(b0, b1)
    local_sum(b1, QF, inner_f)
    f_w0 = start_exchange(fine, 3, [(b1, QF)])

    local_sum(b1, QF, [QF - 1])
    restrict(b1, rw0, True)
    local_sum(rw0, QC, inner_c)
    interior(b1, QF, scaled)
    interior(cinv, QC, invert)
    finish_exchange(rough, 0, [(cinv, QC), (rload, QC)], c_0, [invert, keep])
    apply_coarse(rload, cpow)
    local_sum(cpow, QC, inner_c)
    c_1 = start_exchange(rough, 1, [(cpow, QC), (rw0, QC)])
    interior(cpow, QC, cscaled)

    finish_exchange(fine, 2, [(power, QF)], f_power, [scaled])
    apply_fine(power, power_2)
    local_sum(power_2, QF, inner_f)
    f_power_2 = start_exchange(fine, 4, [(power_2, QF)])
    interior(power_2, QF, scaled)

    finish_exchange(fine, 3, [(b1, QF)], f_w0, [scaled])
    apply_fine(b1, b2)
    local_sum(b2, QF, inner_f)
    f_w1 = start_exchange(fine, 5, [(b2, QF)])

    local_sum(b2, QF, [QF - 1])
    restrict(b2, rw1, True)
    local_sum(rw1, QC, inner_c)
    interior(b2, QF, scaled)
    finish_exchange(rough, 1, [(cpow, QC), (rw0, QC)], c_1, [cscaled, keep])
    apply_coarse(cpow, cpow_2)
    local_sum(cpow_2, QC, inner_c)
    c_2 = start_exchange(rough, 2, [(cpow_2, QC), (rw1, QC)])
    interior(cpow_2, QC, cscaled)
    sum_first = squares(QF, lambda p: power[p])

    finish_exchange(fine, 4, [(power_2, QF)], f_power_2, [scaled])
    sum_second = squares(QF, lambda p: power_2[p])
    line = start_line(0, True, sum_first, sum_second)

    finish_exchange(fine, 5, [(b2, QF)], f_w1, [scaled])
    apply_fine(b2, power)
    restrict(power, rw2, False)
    local_sum(rw2, QC, inner_c)
    c_3 = start_exchange(rough, 3, [(rw2, QC)])

    line = start_line(0, False, *finish_line(0, True, line))
    finish_exchange(rough, 2, [(cpow_2, QC), (rw1, QC)], c_2, [cscaled, keep])
    csum_first = squares(QC, lambda p: cpow[p])
    csum_second = squares(QC, lambda p: cpow_2[p])
    cline = start_line(1, True, csum_first, csum_second)
    scale = coefficients(inverse_estimate(*finish_line(0, False, line)))
    each(
        QF,
        store(smooth, lambda p: scale[0] * b0[p] + scale[1] * b1[p] + scale[2] * b2[p]),
    )
    each(QC, store(crhs, lambda p: rload[p] - (scale[0] * rw0[p] + scale[1] * rw1[p])))

    finish_exchange(rough, 3, [(rw2, QC)], c_3, [keep])
    each(QC, store(crhs, lambda p: crhs[p] - scale[2] * rw2[p]))
    each(QC, store(cb, lambda p: cinv[p] * crhs[p]))
    apply_coarse(cb, cw0)
    local_sum(cw0, QC, inner_c)
    c_4 = start_exchange(rough, 4, [(cw0, QC)])
    interior(cw0, QC, cscaled)
    cline = start_line(1, False, *finish_line(1, True, cline))

    finish_exchange(rough, 4, [(cw0, QC)], c_4, [cscaled])
    apply_coarse(cw0, cw1)
    local_sum(cw1, QC, inner_c)
    c_5 = start_exchange(rough, 5, [(cw1, QC)])
    interior(cw1, QC, cscaled)
    cscale = coefficients(inverse_estimate(*finish_line(1, False, cline)))
    each(QC, store(ccor, lambda p: cscale[0] * cb[p] + cscale[1] * cw0[p]))

    finish_exchange(rough, 5, [(cw1, QC)], c_5, [cscaled])
    each(QC, store(ccor, lambda p: ccor[p] + cscale[2] * cw1[p]))

    def write_planes(dst, q, x, y, values, lane_net):
        for h in range(subs // tile):
            rows = slice(h * tile, (h + 1) * tile)
            for v, block in enumerate(lane_net.merge([value[rows] for value in values])):
                for e in range(group):
                    part = block[e * ey : (e + 1) * ey]
                    dst[v, x, h * group + e, pl.ds(y, ey, stride=q), :] = part

    leaving = []
    cnet = Lanes(QC, tile, ez)
    for x in range(QC):
        for y in range(QC):
            values = [ccor[(x * QC + y) * QC + z] for z in range(QC)]
            write_planes(cresult, QC, x, y, values, cnet)
        for v in range(QC):
            copy = pltpu.make_async_copy(
                cresult.at[v, x], cor_hbm.at[:, x, :, v * ez : (v + 1) * ez], cor_sem.at[v, x]
            )
            copy.start()
            leaving.append(copy)
    for y in range(QC):
        for z in range(QC):
            line = dense(INTERP, [ccor[i * QC * QC + y * QC + z] for i in range(QC)])
            for i in range(QF):
                tmp_a[(i * QC + y) * QC + z] = line[i]
    for x in range(QF):
        for z in range(QC):
            line = dense(INTERP, [tmp_a[(x * QC + i) * QC + z] for i in range(QC)])
            for i in range(QF):
                tmp_b[(x * QF + i) * QC + z] = line[i]
        for y in range(QF):
            line = dense(INTERP, [tmp_b[(x * QF + y) * QC + i] for i in range(QC)])
            values = [smooth[(x * QF + y) * QF + z] + line[z] for z in range(QF)]
            write_planes(result, QF, x, y, values, net)
        for v in range(QF):
            copy = pltpu.make_async_copy(
                result.at[v, x], out_hbm.at[:, x, :, v * ez : (v + 1) * ez], out_sem.at[v, x]
            )
            copy.start()
            leaving.append(copy)
    for copy in pending:
        copy.wait_send()
    for copy in leaving:
        copy.wait()


def on_device(nx, ny, source, conductivity, absorption):
    px, py, pz = source.shape
    ex, ey, ez = px // QF, py // QF, pz // QF
    subs = ex * ey
    face = max(ex, ey)
    f32 = jnp.float32
    dirs = len(DIRS)
    longest = max(nx, ny)
    fine_rows = -(-QF * (QF - 1) * face // 8) * 8
    coarse_rows = -(-2 * QC * (QC - 1) * face // 8) * 8
    scratch = [
        pltpu.VMEM((3, QF, px, py, ez), f32),
        pltpu.VMEM((QF, QF, ex, py, ez), f32),
        pltpu.VMEM((QC, QC, ex, ey * QC, ez), f32),
        *[pltpu.VMEM((QF**3, subs, ez), f32)] * 10,
        pltpu.VMEM((14, QC**3, subs, ez), f32),
        pltpu.VMEM((QF * QF * QC, subs, ez), f32),
        pltpu.VMEM((QF * QF * QC, subs, ez), f32),
        *[pltpu.VMEM((FINE_STAGES, dirs, fine_rows, ez), f32)] * 2,
        *[pltpu.VMEM((COARSE_STAGES, dirs, coarse_rows, ez), f32)] * 2,
        pltpu.VMEM((2, 8, ez), f32),
        pltpu.VMEM((2, nx, 8, ez), f32),
        pltpu.VMEM((2, 8, ez), f32),
        pltpu.VMEM((2, ny, 8, ez), f32),
        pltpu.SemaphoreType.DMA((3, QF)),
        pltpu.SemaphoreType.DMA((QF, QF)),
        pltpu.SemaphoreType.DMA((QC, QC)),
        pltpu.SemaphoreType.DMA((2, FINE_STAGES, dirs)),
        pltpu.SemaphoreType.DMA((2, COARSE_STAGES, dirs)),
        pltpu.SemaphoreType.DMA((2, 2, longest)),
        pltpu.SemaphoreType.DMA((2, nx)),
        pltpu.SemaphoreType.DMA((2, ny)),
    ]
    anywhere = pl.BlockSpec(memory_space=pl.ANY)
    out, cor = pl.pallas_call(
        functools.partial(kernel, nx, ny),
        out_shape=(
            jax.ShapeDtypeStruct((ex, QF, py, pz), f32),
            jax.ShapeDtypeStruct((ex, QC, ey * QC, ez * QC), f32),
        ),
        in_specs=[anywhere] * 3,
        out_specs=(anywhere, anywhere),
        scratch_shapes=scratch,
        compiler_params=pltpu.CompilerParams(
            collective_id=0, has_side_effects=True, vmem_limit_bytes=40 * 1024 * 1024
        ),
    )(source, conductivity, absorption)
    return out.reshape(source.shape), cor.reshape(ex * QC, ey * QC, ez * QC)


def solution(mesh):
    spec = P("gx", "gy", None)
    return jax.shard_map(
        functools.partial(on_device, mesh.shape["gx"], mesh.shape["gy"]),
        mesh=mesh,
        in_specs=(spec,) * 3,
        out_specs=(spec, spec),
        check_vma=False,
    )
```

```python
import functools
import math

import jax
import jax.numpy as jnp
import numpy as np
from jax import lax
from jax.experimental import pallas as pl
from jax.experimental.pallas import tpu as pltpu
from jax.sharding import PartitionSpec as P

SWEEPS = 3
MESH = pl.DeviceIdType.MESH
DIRS = [(-1, -1), (-1, 1), (1, -1), (1, 1), (0, -1), (0, 1), (-1, 0), (1, 0)]
FINE_STAGES, COARSE_STAGES = 6, 6


def deriv_table(points):
    count = len(points)
    barycentric = np.array(
        [
            1.0 / np.prod([points[j] - points[k] for k in range(count) if k != j])
            for j in range(count)
        ]
    )
    table = np.zeros((count, count))
    for i in range(count):
        for j in range(count):
            if i != j:
                table[i, j] = barycentric[j] / (barycentric[i] * (points[i] - points[j]))
        table[i, i] = -np.sum(table[i])
    return table


ROOT = math.sqrt(3.0 / 7.0)
FINE_POINTS = np.array([-1.0, -ROOT, 0.0, ROOT, 1.0])
FINE_W = np.array([0.1, 49.0 / 90.0, 32.0 / 45.0, 49.0 / 90.0, 0.1])
COARSE_POINTS = np.array([-1.0, 0.0, 1.0])
COARSE_W = np.array([1.0 / 3.0, 4.0 / 3.0, 1.0 / 3.0])
FINE_D = deriv_table(FINE_POINTS)
COARSE_D = deriv_table(COARSE_POINTS)
INTERP = np.stack(
    [
        FINE_POINTS * (FINE_POINTS - 1.0) / 2.0,
        1.0 - FINE_POINTS**2,
        FINE_POINTS * (FINE_POINTS + 1.0) / 2.0,
    ],
    1,
)
RESTRICT = INTERP.T * np.array([0.5, 1.0, 1.0, 1.0, 0.5])[None, :]
TRANSFER = INTERP.T
QF, QC = 5, 3


def chebyshev_coefficients():
    theta, delta, sigma, rho = 0.75, 0.45, 5.0 / 3.0, 0.6
    x = np.zeros(SWEEPS + 1)
    r = np.zeros(SWEEPS + 1)
    r[0] = 1.0
    d = r / theta
    for sweep in range(SWEEPS):
        x = x + d
        r = r - np.concatenate([[0.0], d[:-1]])
        if sweep + 1 < SWEEPS:
            rho_next = 1.0 / (2.0 * sigma - rho)
            d = rho_next * rho * d + 2.0 * rho_next / delta * r
            rho = rho_next
    return [float(v) for v in x[:SWEEPS]]


CHEB = chebyshev_coefficients()


def antisym(table, u):
    n = len(u)
    half = n // 2
    even = [u[j] + u[n - 1 - j] for j in range(half)]
    odd = [u[j] - u[n - 1 - j] for j in range(half)]
    out = [None] * n
    for i in range(half):
        p = float(table[i, half]) * u[half]
        q = None
        for j in range(half):
            s = (table[i, j] + table[i, n - 1 - j]) / 2
            t = (table[i, j] - table[i, n - 1 - j]) / 2
            p = p + float(s) * even[j]
            q = float(t) * odd[j] if q is None else q + float(t) * odd[j]
        out[i] = q + p
        out[n - 1 - i] = q - p
    mid = None
    for j in range(half):
        term = float(table[half, j]) * odd[j]
        mid = term if mid is None else mid + term
    out[half] = mid
    return out


def dense(table, u):
    out = []
    for i in range(table.shape[0]):
        acc = None
        for j in range(table.shape[1]):
            c = float(table[i, j])
            if abs(c) < 1e-14:
                continue
            term = u[j] if c == 1.0 else c * u[j]
            acc = term if acc is None else acc + term
        out.append(acc)
    return out


def plane_starts(q, axis, a, b):
    strides = (q * q, q, 1)
    other = [s for k, s in enumerate(strides) if k != axis]
    return a * other[0] + b * other[1], strides[axis]


def z_sum(line, lanes):
    lo, hi = line[0], line[-1]
    line[-1] = hi + pltpu.roll(lo, lanes - 1, 1)
    line[0] = lo + pltpu.roll(hi, 1, 1)
    return line


def local_op(src, dst, flux, mass, table, lanes):
    q = table.shape[0]

    def lines(axis, a):
        def read(b):
            start, step = plane_starts(q, axis, a, b)
            u = [src[start + step * i] for i in range(q)]
            base = None if axis == 0 else [dst[start + step * i] for i in range(q)]
            return u, base

        ahead = read(0)
        for b in range(q):
            u, base = ahead
            if b + 1 < q:
                ahead = read(b + 1)
            start, step = plane_starts(q, axis, a, b)
            g = antisym(table, u)
            g = [flux[start + step * i] * g[i] for i in range(q)]
            r = antisym(table.T, g)
            for i in range(q):
                r[i] = (mass[start + step * i] * u[i] if base is None else base[i]) + r[i]
            if axis == 2:
                r = z_sum(r, lanes)
            for i in range(q):
                dst[start + step * i] = r[i]

    for axis in range(2):

        @pl.loop(0, q)
        def _(a, axis=axis):
            lines(axis, a)

    for a in range(q):
        lines(2, a)


def local_diag(dst, flux, mass, table, lanes):
    q = table.shape[0]
    square = (table * table).T

    def lines(axis, a):
        for b in range(q):
            start, step = plane_starts(q, axis, a, b)
            r = dense(square, [flux[start + step * i] for i in range(q)])
            for i in range(q):
                base = mass if axis == 0 else dst
                r[i] = base[start + step * i] + r[i]
            if axis == 2:
                r = z_sum(r, lanes)
            for i in range(q):
                dst[start + step * i] = r[i]

    for axis in range(2):

        @pl.loop(0, q)
        def _(a, axis=axis):
            lines(axis, a)

    for a in range(q):
        lines(2, a)


class Lanes:
    def __init__(self, q, rows, ez):
        self.q = q
        lane = lax.broadcasted_iota(jnp.int32, (rows, ez), 1)
        self.turn = ez % q
        self.back = pow(self.turn, -1, q)
        unit = pow(q, -1, ez)
        self.pick = [lax.rem(lane * q + k, ez) for k in range(q)]
        self.place = [lax.rem((lane + (ez - k)) * unit, ez) for k in range(q)]
        s = lax.rem(lane, q)
        self.out_steps = self.bits(s, q - self.back)
        self.in_steps = self.bits(s, self.back)

    def bits(self, s, by):
        amount = lax.rem(s * by, self.q)
        steps, step = [], 1
        while step < self.q:
            steps.append((step, lax.rem(lax.div(amount, step), 2) == 1))
            step *= 2
        return steps

    def select(self, blocks, steps):
        for step, mask in steps:
            blocks = [
                jnp.where(mask, blocks[(v + step) % self.q], blocks[v]) for v in range(self.q)
            ]
        return blocks

    def mix(self, blocks):
        mixed = self.select(blocks, self.out_steps)
        return [mixed[self.back * k % self.q] for k in range(self.q)]

    def unmix(self, placed):
        return self.select([placed[self.turn * j % self.q] for j in range(self.q)], self.in_steps)


def kernel(
    nx,
    ny,
    src_hbm,
    cond_hbm,
    abs_hbm,
    out_hbm,
    cor_hbm,
    stored,
    result,
    cresult,
    load,
    inv,
    power,
    power_2,
    b0,
    b1,
    b2,
    flux,
    mass,
    smooth,
    coarse,
    tmp_a,
    tmp_b,
    fine_send,
    fine_recv,
    coarse_send,
    coarse_recv,
    line_x_send,
    line_x,
    line_y_send,
    line_y,
    in_sem,
    out_sem,
    cor_sem,
    fine_sems,
    coarse_sems,
    line_send_sem,
    line_x_sem,
    line_y_sem,
):
    px, py, pz = src_hbm.shape
    ex, ey, ez = px // QF, py // QF, pz // QF
    subs, lanes = ex * ey, ez
    tile = 8
    mx, my = lax.axis_index("gx"), lax.axis_index("gy")

    def target(dx, dy):
        return (lax.rem(mx + dx + nx, nx), lax.rem(my + dy + ny, ny))

    greeted = {(o, 0) for o in range(1, nx)} | {(0, o) for o in range(1, ny)}
    greeted |= {(dx % nx, dy % ny) for dx, dy in DIRS}
    greeted = sorted(greeted)
    barrier = pltpu.get_barrier_semaphore()
    for dx, dy in greeted:
        pl.semaphore_signal(barrier, inc=1, device_id=target(dx, dy), device_id_type=MESH)

    arriving = []
    for n, ref in enumerate((src_hbm, cond_hbm, abs_hbm)):
        for v in range(QF):
            copy = pltpu.make_async_copy(
                ref.at[:, :, v * ez : (v + 1) * ez], stored.at[n, v], in_sem.at[n, v]
            )
            copy.start()
            arriving.append(copy)

    sub = lax.broadcasted_iota(jnp.int32, (subs, lanes), 0)
    row_y = lax.rem(sub, ey)
    first_x, last_x = sub < ey, sub >= (ex - 1) * ey
    first_y, last_y = row_y == 0, row_y == ey - 1

    def shifted(plane, shift):
        return pltpu.roll(plane, shift % subs, 0)

    def local_sum(ref, q, zs):
        last = q - 1
        for z in zs:
            for y in range(q):
                p, r = y * q + z, (last * q + y) * q + z
                lo, hi = ref[p], ref[r]
                ref[p] = jnp.where(first_x, lo, lo + shifted(hi, ey))
                ref[r] = jnp.where(last_x, hi, hi + shifted(lo, -ey))
            for x in range(q):
                p, r = x * q * q + z, (x * q + last) * q + z
                lo, hi = ref[p], ref[r]
                ref[p] = jnp.where(first_y, lo, lo + shifted(hi, 1))
                ref[r] = jnp.where(last_y, hi, hi + shifted(lo, -1))

    def edge(dx, dy, q):
        xs = range(q) if dx == 0 else [0 if dx < 0 else q - 1]
        ys = range(q) if dy == 0 else [0 if dy < 0 else q - 1]
        planes = [(x * q + y) * q + z for x in xs for y in ys for z in range(q - 1)]
        e, f = (0 if dx < 0 else ex - 1), (0 if dy < 0 else ey - 1)
        if dy == 0:
            return planes, ey, slice(e * ey, (e + 1) * ey)
        if dx == 0:
            return planes, ex, pl.ds(f, ex, stride=ey)
        return planes, 1, slice(e * ey + f, e * ey + f + 1)

    def whole_rows(count):
        return -(-count // tile) * tile

    pending = []

    def start_exchange(level, stage, fields):
        send, recv, sems = level
        copies = []
        for d, (dx, dy) in enumerate(DIRS):
            at = 0
            for ref, q in fields:
                planes, count, rows = edge(dx, dy, q)
                for p in planes:
                    send[stage, d, at : at + count, :] = ref[p, rows, :]
                    at += count
            total = whole_rows(at)
            copy = pltpu.make_async_remote_copy(
                src_ref=send.at[stage, d, pl.ds(0, total)],
                dst_ref=recv.at[stage, d, pl.ds(0, total)],
                send_sem=sems.at[0, stage, d],
                recv_sem=sems.at[1, stage, d],
                device_id=target(dx, dy),
                device_id_type=MESH,
            )
            copy.start()
            copies.append(copy)
        return copies

    def finish_exchange(level, stage, fields, copies, finals):
        _, recv, _ = level
        for d in reversed(range(len(DIRS))):
            dx, dy = DIRS[d]
            copies[d].wait_recv()
            at = 0
            for ref, q in fields:
                planes, count, rows = edge(-dx, -dy, q)
                for p in planes:
                    ref[p, rows, :] = ref[p, rows, :] + recv[stage, d, at : at + count, :]
                    at += count
        pending.extend(copies)
        for (ref, q), final in zip(fields, finals):
            for x in range(q):
                for y in range(q):
                    if x in (0, q - 1) or y in (0, q - 1):
                        p = (x * q + y) * q
                        for z in range(q - 1):
                            value = final(p + z, ref[p + z])
                            ref[p + z] = value
                            if z == 0:
                                ref[p + q - 1] = pltpu.roll(value, lanes - 1, 1)

    def interior(ref, q, final):
        for x in range(1, q - 1):
            for y in range(1, q - 1):
                for z in range(q):
                    p = (x * q + y) * q + z
                    ref[p] = final(p, ref[p])

    fine = (fine_send, fine_recv, fine_sems)
    rough = (coarse_send, coarse_recv, coarse_sems)

    def start_line(which, along_x, first, second):
        out, slots, sems = (
            (line_x_send, line_x, line_x_sem) if along_x else (line_y_send, line_y, line_y_sem)
        )
        count = nx if along_x else ny
        out[which, 0:1] = first
        out[which, 1:2] = second
        copies = []
        for o in range(1, count):
            copy = pltpu.make_async_remote_copy(
                src_ref=out.at[which],
                dst_ref=slots.at[which, o],
                send_sem=line_send_sem.at[which, 0 if along_x else 1, o],
                recv_sem=sems.at[which, o],
                device_id=target(o, 0) if along_x else target(0, o),
                device_id_type=MESH,
            )
            copy.start()
            copies.append(copy)
        return copies

    def finish_line(which, along_x, copies):
        out, slots = (line_x_send, line_x) if along_x else (line_y_send, line_y)
        count = nx if along_x else ny
        for copy in copies:
            copy.wait_recv()
        pending.extend(copies)
        total = out[which]
        for o in range(1, count):
            total = total + slots[which, o]
        return total[0:1], total[1:2]

    def inverse_estimate(first, second):
        first = jnp.sum(first, axis=1, keepdims=True)
        second = jnp.sum(second, axis=1, keepdims=True)
        return 1.0 / jnp.sqrt(second / (first + 1e-06))

    def coefficients(inv_est):
        power = inv_est
        out = []
        for c in CHEB:
            out.append(jnp.broadcast_to(c * power, (subs, lanes)))
            power = power * inv_est
        return out

    net = Lanes(QF, tile, ez)
    group = tile // ey

    def permuted(plane, index):
        tiles = [
            jnp.take_along_axis(plane[h * tile : (h + 1) * tile], index, axis=1)
            for h in range(subs // tile)
        ]
        return jnp.concatenate(tiles, axis=0)

    def read_planes(n, dst):
        for x in range(QF):
            for y in range(QF):
                for h in range(subs // tile):
                    blocks = []
                    for v in range(QF):
                        parts = [
                            stored[n, v, (h * group + e) * QF + x, pl.ds(y, ey, stride=QF), :]
                            for e in range(group)
                        ]
                        blocks.append(jnp.concatenate(parts, axis=0))
                    for z, block in enumerate(net.mix(blocks)):
                        dst[(x * QF + y) * QF + z, h * tile : (h + 1) * tile, :] = block

    (
        cflux,
        cmass,
        cinv,
        rload,
        cpow,
        cpow_2,
        rw0,
        rw1,
        rw2,
        crhs,
        cb,
        cw0,
        cw1,
        ccor,
    ) = [coarse.at[i] for i in range(14)]

    for copy in arriving[:QF]:
        copy.wait()
    read_planes(0, load)
    for z in range(QF):
        for x in range(QF):
            for y in range(QF):
                p = (x * QF + y) * QF + z
                load[p] = float(FINE_W[x] * FINE_W[y] * FINE_W[z]) * permuted(load[p], net.pick[z])
    for a in range(QF * QF):
        line = z_sum([load[a * QF], load[a * QF + QF - 1]], lanes)
        load[a * QF] = line[0]
        load[a * QF + QF - 1] = line[1]
    local_sum(load, QF, range(QF - 1))

    def each(q, body):
        @pl.loop(0, q * q)
        def _(a):
            for i in range(q):
                body(a * q + i)

    def squares(q, values):
        def body(a, acc):
            for i in range(q):
                v = values(a * q + i)
                acc = acc + v * v
            return acc

        total = lax.fori_loop(0, q * q, body, jnp.zeros((subs, lanes), jnp.float32))
        return jnp.sum(total, axis=0, keepdims=True)

    def store(dst, values):
        def body(p):
            dst[p] = values(p)

        return body

    def half_unless(mask):
        return jnp.where(mask, 1.0, 0.5)

    def weighted(line, ends):
        if ends is None:
            return line
        return [half_unless(ends[0]) * line[0]] + line[1:-1] + [half_unless(ends[1]) * line[-1]]

    def restrict(field, dst, summed):
        ends_x = (first_x, last_x) if summed else None
        ends_y = (first_y, last_y) if summed else None

        @pl.loop(0, QF)
        def _(a):
            for c in range(QF):
                line = [field[i * QF * QF + a * QF + c] for i in range(QF)]
                line = dense(TRANSFER, weighted(line, ends_x))
                for i in range(QC):
                    tmp_a[i * QF * QF + a * QF + c] = line[i]

        for a in range(QC):
            for c in range(QF):
                line = [tmp_a[a * QF * QF + i * QF + c] for i in range(QF)]
                line = dense(TRANSFER, weighted(line, ends_y))
                for i in range(QC):
                    tmp_b[a * QC * QF + i * QF + c] = line[i]

        for a in range(QC):
            for c in range(QC):
                line = dense(RESTRICT, [tmp_b[a * QC * QF + c * QF + i] for i in range(QF)])
                line = z_sum(line, lanes)
                for i in range(QC):
                    dst[a * QC * QC + c * QC + i] = line[i]

    def apply_fine(src, dst):
        local_op(src, dst, flux, mass, FINE_D, lanes)

    def apply_coarse(src, dst):
        local_op(src, dst, cflux, cmass, COARSE_D, lanes)

    keep = lambda p, v: v
    invert = lambda p, v: 1.0 / v
    scaled = lambda p, v: inv[p] * v
    cscaled = lambda p, v: cinv[p] * v
    inner_f, inner_c = range(QF - 1), range(QC - 1)

    pl.semaphore_wait(barrier, len(greeted))
    f_load = start_exchange(fine, 0, [(load, QF)])

    pick = {0: 0, 2: 1, 4: 2}
    for n, full, part in ((1, flux, cflux), (2, mass, cmass)):
        for copy in arriving[n * QF : (n + 1) * QF]:
            copy.wait()
        read_planes(n, full)
        for z in range(QF):
            for x in range(QF):
                for y in range(QF):
                    p = (x * QF + y) * QF + z
                    value = permuted(full[p], net.pick[z])
                    full[p] = float(FINE_W[x] * FINE_W[y] * FINE_W[z]) * value
                    if x in pick and y in pick and z in pick:
                        i, j, k = pick[x], pick[y], pick[z]
                        weight = float(COARSE_W[i] * COARSE_W[j] * COARSE_W[k])
                        part[(i * QC + j) * QC + k] = weight * value

    local_diag(inv, flux, mass, FINE_D, lanes)
    local_sum(inv, QF, inner_f)
    f_diag = start_exchange(fine, 1, [(inv, QF)])

    local_sum(load, QF, [QF - 1])
    restrict(load, rload, True)
    local_sum(rload, QC, inner_c)
    local_diag(cinv, cflux, cmass, COARSE_D, lanes)
    local_sum(cinv, QC, inner_c)
    c_0 = start_exchange(rough, 0, [(cinv, QC), (rload, QC)])
    interior(inv, QF, invert)

    finish_exchange(fine, 0, [(load, QF)], f_load, [keep])
    apply_fine(load, power)
    local_sum(power, QF, inner_f)
    f_power = start_exchange(fine, 2, [(power, QF)])
    interior(power, QF, scaled)

    finish_exchange(fine, 1, [(inv, QF)], f_diag, [invert])
    each(QF, store(b0, lambda p: inv[p] * load[p]))
    apply_fine(b0, b1)
    local_sum(b1, QF, inner_f)
    f_w0 = start_exchange(fine, 3, [(b1, QF)])

    local_sum(b1, QF, [QF - 1])
    restrict(b1, rw0, True)
    local_sum(rw0, QC, inner_c)
    interior(b1, QF, scaled)
    interior(cinv, QC, invert)
    finish_exchange(rough, 0, [(cinv, QC), (rload, QC)], c_0, [invert, keep])
    apply_coarse(rload, cpow)
    local_sum(cpow, QC, inner_c)
    c_1 = start_exchange(rough, 1, [(cpow, QC), (rw0, QC)])
    interior(cpow, QC, cscaled)

    finish_exchange(fine, 2, [(power, QF)], f_power, [scaled])
    apply_fine(power, power_2)
    local_sum(power_2, QF, inner_f)
    f_power_2 = start_exchange(fine, 4, [(power_2, QF)])
    interior(power_2, QF, scaled)

    finish_exchange(fine, 3, [(b1, QF)], f_w0, [scaled])
    apply_fine(b1, b2)
    local_sum(b2, QF, inner_f)
    f_w1 = start_exchange(fine, 5, [(b2, QF)])

    local_sum(b2, QF, [QF - 1])
    restrict(b2, rw1, True)
    local_sum(rw1, QC, inner_c)
    interior(b2, QF, scaled)
    finish_exchange(rough, 1, [(cpow, QC), (rw0, QC)], c_1, [cscaled, keep])
    apply_coarse(cpow, cpow_2)
    local_sum(cpow_2, QC, inner_c)
    c_2 = start_exchange(rough, 2, [(cpow_2, QC), (rw1, QC)])
    interior(cpow_2, QC, cscaled)
    sum_first = squares(QF, lambda p: power[p])

    finish_exchange(fine, 4, [(power_2, QF)], f_power_2, [scaled])
    sum_second = squares(QF, lambda p: power_2[p])
    line = start_line(0, True, sum_first, sum_second)

    finish_exchange(fine, 5, [(b2, QF)], f_w1, [scaled])
    line = start_line(0, False, *finish_line(0, True, line))
    apply_fine(b2, power)
    restrict(power, rw2, False)
    local_sum(rw2, QC, inner_c)
    c_3 = start_exchange(rough, 3, [(rw2, QC)])

    finish_exchange(rough, 2, [(cpow_2, QC), (rw1, QC)], c_2, [cscaled, keep])
    csum_first = squares(QC, lambda p: cpow[p])
    csum_second = squares(QC, lambda p: cpow_2[p])
    cline = start_line(1, True, csum_first, csum_second)
    scale = coefficients(inverse_estimate(*finish_line(0, False, line)))
    each(
        QF,
        store(smooth, lambda p: scale[0] * b0[p] + scale[1] * b1[p] + scale[2] * b2[p]),
    )
    each(QC, store(crhs, lambda p: rload[p] - (scale[0] * rw0[p] + scale[1] * rw1[p])))

    finish_exchange(rough, 3, [(rw2, QC)], c_3, [keep])
    each(QC, store(crhs, lambda p: crhs[p] - scale[2] * rw2[p]))
    each(QC, store(cb, lambda p: cinv[p] * crhs[p]))
    apply_coarse(cb, cw0)
    local_sum(cw0, QC, inner_c)
    c_4 = start_exchange(rough, 4, [(cw0, QC)])
    interior(cw0, QC, cscaled)
    cline = start_line(1, False, *finish_line(1, True, cline))

    finish_exchange(rough, 4, [(cw0, QC)], c_4, [cscaled])
    apply_coarse(cw0, cw1)
    local_sum(cw1, QC, inner_c)
    c_5 = start_exchange(rough, 5, [(cw1, QC)])
    interior(cw1, QC, cscaled)
    cscale = coefficients(inverse_estimate(*finish_line(1, False, cline)))
    each(QC, store(ccor, lambda p: cscale[0] * cb[p] + cscale[1] * cw0[p]))

    finish_exchange(rough, 5, [(cw1, QC)], c_5, [cscaled])
    each(QC, store(ccor, lambda p: ccor[p] + cscale[2] * cw1[p]))

    def write_planes(dst, planes, q, lane_net):
        for x in range(q):
            for y in range(q):
                for h in range(subs // tile):
                    rows = slice(h * tile, (h + 1) * tile)
                    placed = [planes[(x * q + y) * q + z, rows, :] for z in range(q)]
                    for v, block in enumerate(lane_net.unmix(placed)):
                        for e in range(group):
                            part = block[e * ey : (e + 1) * ey]
                            dst[v, x, h * group + e, pl.ds(y, ey, stride=q), :] = part

    leaving = []
    cnet = Lanes(QC, tile, ez)
    for z in range(QC):
        for a in range(QC * QC):
            tmp_b[a * QC + z] = permuted(ccor[a * QC + z], cnet.place[z])
    write_planes(cresult, tmp_b, QC, cnet)
    for v in range(QC):
        for x in range(QC):
            copy = pltpu.make_async_copy(
                cresult.at[v, x], cor_hbm.at[:, x, :, v * ez : (v + 1) * ez], cor_sem.at[v, x]
            )
            copy.start()
            leaving.append(copy)
    for y in range(QC):
        for z in range(QC):
            line = dense(INTERP, [ccor[i * QC * QC + y * QC + z] for i in range(QC)])
            for i in range(QF):
                tmp_a[(i * QC + y) * QC + z] = line[i]
    for x in range(QF):
        for z in range(QC):
            line = dense(INTERP, [tmp_a[(x * QC + i) * QC + z] for i in range(QC)])
            for i in range(QF):
                tmp_b[(x * QF + i) * QC + z] = line[i]
    for z in range(QF):
        for a in range(QF * QF):
            p = a * QF + z
            lifted = dense(INTERP[z : z + 1], [tmp_b[a * QC + i] for i in range(QC)])[0]
            smooth[p] = permuted(smooth[p] + lifted, net.place[z])
    write_planes(result, smooth, QF, net)
    for v in range(QF):
        for x in range(QF):
            copy = pltpu.make_async_copy(
                result.at[v, x], out_hbm.at[:, x, :, v * ez : (v + 1) * ez], out_sem.at[v, x]
            )
            copy.start()
            leaving.append(copy)
    for copy in pending:
        copy.wait_send()
    for copy in leaving:
        copy.wait()


def on_device(nx, ny, source, conductivity, absorption):
    px, py, pz = source.shape
    ex, ey, ez = px // QF, py // QF, pz // QF
    subs = ex * ey
    face = max(ex, ey)
    f32 = jnp.float32
    dirs = len(DIRS)
    longest = max(nx, ny)
    fine_rows = -(-QF * (QF - 1) * face // 8) * 8
    coarse_rows = -(-2 * QC * (QC - 1) * face // 8) * 8
    scratch = [
        pltpu.VMEM((3, QF, px, py, ez), f32),
        pltpu.VMEM((QF, QF, ex, py, ez), f32),
        pltpu.VMEM((QC, QC, ex, ey * QC, ez), f32),
        *[pltpu.VMEM((QF**3, subs, ez), f32)] * 10,
        pltpu.VMEM((14, QC**3, subs, ez), f32),
        pltpu.VMEM((QF * QF * QC, subs, ez), f32),
        pltpu.VMEM((QF * QF * QC, subs, ez), f32),
        *[pltpu.VMEM((FINE_STAGES, dirs, fine_rows, ez), f32)] * 2,
        *[pltpu.VMEM((COARSE_STAGES, dirs, coarse_rows, ez), f32)] * 2,
        pltpu.VMEM((2, 8, ez), f32),
        pltpu.VMEM((2, nx, 8, ez), f32),
        pltpu.VMEM((2, 8, ez), f32),
        pltpu.VMEM((2, ny, 8, ez), f32),
        pltpu.SemaphoreType.DMA((3, QF)),
        pltpu.SemaphoreType.DMA((QF, QF)),
        pltpu.SemaphoreType.DMA((QC, QC)),
        pltpu.SemaphoreType.DMA((2, FINE_STAGES, dirs)),
        pltpu.SemaphoreType.DMA((2, COARSE_STAGES, dirs)),
        pltpu.SemaphoreType.DMA((2, 2, longest)),
        pltpu.SemaphoreType.DMA((2, nx)),
        pltpu.SemaphoreType.DMA((2, ny)),
    ]
    anywhere = pl.BlockSpec(memory_space=pl.ANY)
    out, cor = pl.pallas_call(
        functools.partial(kernel, nx, ny),
        out_shape=(
            jax.ShapeDtypeStruct((ex, QF, py, pz), f32),
            jax.ShapeDtypeStruct((ex, QC, ey * QC, ez * QC), f32),
        ),
        in_specs=[pl.BlockSpec(memory_space=pltpu.HBM)] * 3,
        out_specs=(anywhere, anywhere),
        scratch_shapes=scratch,
        compiler_params=pltpu.CompilerParams(
            collective_id=0, has_side_effects=True, vmem_limit_bytes=52 * 1024 * 1024
        ),
    )(source, conductivity, absorption)
    return out.reshape(source.shape), cor.reshape(ex * QC, ey * QC, ez * QC)


def solution(mesh):
    spec = P("gx", "gy", None)
    return jax.shard_map(
        functools.partial(on_device, mesh.shape["gx"], mesh.shape["gy"]),
        mesh=mesh,
        in_specs=(spec,) * 3,
        out_specs=(spec, spec),
        check_vma=False,
    )
```

```python
import functools
import math

import jax
import jax.numpy as jnp
import numpy as np
from jax import lax
from jax.experimental import pallas as pl
from jax.experimental.pallas import tpu as pltpu
from jax.sharding import PartitionSpec as P

SWEEPS = 3
MESH = pl.DeviceIdType.MESH
DIRS = [(-1, -1), (-1, 1), (1, -1), (1, 1), (0, -1), (0, 1), (-1, 0), (1, 0)]
FINE_STAGES, COARSE_STAGES = 6, 6


def deriv_table(points):
    count = len(points)
    barycentric = np.array(
        [
            1.0 / np.prod([points[j] - points[k] for k in range(count) if k != j])
            for j in range(count)
        ]
    )
    table = np.zeros((count, count))
    for i in range(count):
        for j in range(count):
            if i != j:
                table[i, j] = barycentric[j] / (barycentric[i] * (points[i] - points[j]))
        table[i, i] = -np.sum(table[i])
    return table


ROOT = math.sqrt(3.0 / 7.0)
FINE_POINTS = np.array([-1.0, -ROOT, 0.0, ROOT, 1.0])
FINE_W = np.array([0.1, 49.0 / 90.0, 32.0 / 45.0, 49.0 / 90.0, 0.1])
COARSE_POINTS = np.array([-1.0, 0.0, 1.0])
COARSE_W = np.array([1.0 / 3.0, 4.0 / 3.0, 1.0 / 3.0])
FINE_D = deriv_table(FINE_POINTS)
COARSE_D = deriv_table(COARSE_POINTS)
INTERP = np.stack(
    [
        FINE_POINTS * (FINE_POINTS - 1.0) / 2.0,
        1.0 - FINE_POINTS**2,
        FINE_POINTS * (FINE_POINTS + 1.0) / 2.0,
    ],
    1,
)
RESTRICT = INTERP.T * np.array([0.5, 1.0, 1.0, 1.0, 0.5])[None, :]
TRANSFER = INTERP.T
QF, QC = 5, 3


def chebyshev_coefficients():
    theta, delta, sigma, rho = 0.75, 0.45, 5.0 / 3.0, 0.6
    x = np.zeros(SWEEPS + 1)
    r = np.zeros(SWEEPS + 1)
    r[0] = 1.0
    d = r / theta
    for sweep in range(SWEEPS):
        x = x + d
        r = r - np.concatenate([[0.0], d[:-1]])
        if sweep + 1 < SWEEPS:
            rho_next = 1.0 / (2.0 * sigma - rho)
            d = rho_next * rho * d + 2.0 * rho_next / delta * r
            rho = rho_next
    return [float(v) for v in x[:SWEEPS]]


CHEB = chebyshev_coefficients()


def antisym(table, u):
    n = len(u)
    half = n // 2
    even = [u[j] + u[n - 1 - j] for j in range(half)]
    odd = [u[j] - u[n - 1 - j] for j in range(half)]
    out = [None] * n
    for i in range(half):
        p = float(table[i, half]) * u[half]
        q = None
        for j in range(half):
            s = (table[i, j] + table[i, n - 1 - j]) / 2
            t = (table[i, j] - table[i, n - 1 - j]) / 2
            p = p + float(s) * even[j]
            q = float(t) * odd[j] if q is None else q + float(t) * odd[j]
        out[i] = q + p
        out[n - 1 - i] = q - p
    mid = None
    for j in range(half):
        term = float(table[half, j]) * odd[j]
        mid = term if mid is None else mid + term
    out[half] = mid
    return out


def dense(table, u):
    out = []
    for i in range(table.shape[0]):
        acc = None
        for j in range(table.shape[1]):
            c = float(table[i, j])
            if abs(c) < 1e-14:
                continue
            term = u[j] if c == 1.0 else c * u[j]
            acc = term if acc is None else acc + term
        out.append(acc)
    return out


def centrosym(table, u):
    n = len(u)
    half = n // 2
    even = [u[j] + u[n - 1 - j] for j in range(half)]
    odd = [u[j] - u[n - 1 - j] for j in range(half)]
    out = [None] * n
    for i in range(half):
        s = [(table[i, j] + table[i, n - 1 - j]) / 2 for j in range(half)]
        t = [[(table[i, j] - table[i, n - 1 - j]) / 2 for j in range(half)]]
        p = dense(np.array([s + [table[i, half]]]), even + [u[half]])[0]
        q = dense(np.array(t), odd)[0]
        out[i] = p + q
        out[n - 1 - i] = p - q
    middle = np.array([[table[half, j] for j in range(half + 1)]])
    out[half] = dense(middle, even + [u[half]])[0]
    return out


def plane_starts(q, axis, a, b):
    strides = (q * q, q, 1)
    other = [s for k, s in enumerate(strides) if k != axis]
    return a * other[0] + b * other[1], strides[axis]


def z_sum(line, lanes):
    lo, hi = line[0], line[-1]
    line[-1] = hi + pltpu.roll(lo, lanes - 1, 1)
    line[0] = lo + pltpu.roll(hi, 1, 1)
    return line


def local_op(src, dst, flux, mass, table, lanes, between=None):
    q = table.shape[0]

    def lines(axis, places):
        def read(n):
            start, step = plane_starts(q, axis, *places[n])
            u = [src[start + step * i] for i in range(q)]
            base = None if axis == 0 else [dst[start + step * i] for i in range(q)]
            return u, base

        ahead = read(0)
        for n in range(len(places)):
            u, base = ahead
            if n + 1 < len(places):
                ahead = read(n + 1)
            start, step = plane_starts(q, axis, *places[n])
            g = antisym(table, u)
            g = [flux[start + step * i] * g[i] for i in range(q)]
            r = antisym(table.T, g)
            for i in range(q):
                r[i] = (mass[start + step * i] * u[i] if base is None else base[i]) + r[i]
            if axis == 2:
                r = z_sum(r, lanes)
            for i in range(q):
                dst[start + step * i] = r[i]

    for axis in range(2):

        @pl.loop(0, q)
        def _(a, axis=axis):
            lines(axis, [(a, b) for b in range(q)])

    lines(2, [(a, b) for b in (0, q - 1) for a in range(q)])
    if between is not None:
        between()
    lines(2, [(a, b) for b in range(1, q - 1) for a in (0, q - 1)])
    lines(2, [(a, b) for b in range(1, q - 1) for a in range(1, q - 1)])


def local_diag(dst, flux, mass, table, lanes):
    q = table.shape[0]
    square = (table * table).T

    def lines(axis, a):
        for b in range(q):
            start, step = plane_starts(q, axis, a, b)
            r = centrosym(square, [flux[start + step * i] for i in range(q)])
            for i in range(q):
                base = mass if axis == 0 else dst
                r[i] = base[start + step * i] + r[i]
            if axis == 2:
                r = z_sum(r, lanes)
            for i in range(q):
                dst[start + step * i] = r[i]

    for axis in range(2):

        @pl.loop(0, q)
        def _(a, axis=axis):
            lines(axis, a)

    for a in range(q):
        lines(2, a)


class Lanes:
    def __init__(self, q, rows, ez):
        self.q = q
        lane = lax.broadcasted_iota(jnp.int32, (rows, ez), 1)
        self.turn = ez % q
        self.back = pow(self.turn, -1, q)
        unit = pow(q, -1, ez)
        self.pick = [lax.rem(lane * q + k, ez) for k in range(q)]
        self.place = [lax.rem((lane + (ez - k)) * unit, ez) for k in range(q)]
        s = lax.rem(lane, q)
        self.out_steps = self.bits(s, q - self.back)
        self.in_steps = self.bits(s, self.back)

    def bits(self, s, by):
        amount = lax.rem(s * by, self.q)
        steps, step = [], 1
        while step < self.q:
            steps.append((step, lax.rem(lax.div(amount, step), 2) == 1))
            step *= 2
        return steps

    def select(self, blocks, steps):
        for step, mask in steps:
            blocks = [
                jnp.where(mask, blocks[(v + step) % self.q], blocks[v]) for v in range(self.q)
            ]
        return blocks

    def mix(self, blocks):
        mixed = self.select(blocks, self.out_steps)
        return [mixed[self.back * k % self.q] for k in range(self.q)]

    def unmix(self, placed):
        return self.select([placed[self.turn * j % self.q] for j in range(self.q)], self.in_steps)


def kernel(
    nx,
    ny,
    src_hbm,
    cond_hbm,
    abs_hbm,
    out_hbm,
    cor_hbm,
    stored,
    result,
    cresult,
    load,
    inv,
    power,
    power_2,
    b0,
    b1,
    b2,
    flux,
    mass,
    smooth,
    coarse,
    tmp_a,
    tmp_b,
    fine_send,
    fine_recv,
    coarse_send,
    coarse_recv,
    line_x_send,
    line_x,
    line_y_send,
    line_y,
    in_sem,
    out_sem,
    cor_sem,
    fine_sems,
    coarse_sems,
    line_send_sem,
    line_x_sem,
    line_y_sem,
):
    px, py, pz = src_hbm.shape
    ex, ey, ez = px // QF, py // QF, pz // QF
    subs, lanes = ex * ey, ez
    tile = 8
    mx, my = lax.axis_index("gx"), lax.axis_index("gy")

    def target(dx, dy):
        return (lax.rem(mx + dx + nx, nx), lax.rem(my + dy + ny, ny))

    greeted = {(o, 0) for o in range(1, nx)} | {(0, o) for o in range(1, ny)}
    greeted |= {(dx % nx, dy % ny) for dx, dy in DIRS}
    greeted = sorted(greeted)
    barrier = pltpu.get_barrier_semaphore()
    for dx, dy in greeted:
        pl.semaphore_signal(barrier, inc=1, device_id=target(dx, dy), device_id_type=MESH)

    arriving = []
    for n, ref in enumerate((src_hbm, cond_hbm, abs_hbm)):
        for v in range(QF):
            copy = pltpu.make_async_copy(
                ref.at[:, :, v * ez : (v + 1) * ez], stored.at[n, v], in_sem.at[n, v]
            )
            copy.start()
            arriving.append(copy)

    sub = lax.broadcasted_iota(jnp.int32, (subs, lanes), 0)
    row_y = lax.rem(sub, ey)
    first_x, last_x = sub < ey, sub >= (ex - 1) * ey
    first_y, last_y = row_y == 0, row_y == ey - 1

    def shifted(plane, shift):
        return pltpu.roll(plane, shift % subs, 0)

    def sum_x(ref, q, zs, ys):
        last = q - 1
        for z in zs:
            for y in ys:
                p, r = y * q + z, (last * q + y) * q + z
                lo, hi = ref[p], ref[r]
                ref[p] = jnp.where(first_x, lo, lo + shifted(hi, ey))
                ref[r] = jnp.where(last_x, hi, hi + shifted(lo, -ey))

    def sum_y(ref, q, zs):
        last = q - 1
        for z in zs:
            for x in range(q):
                p, r = x * q * q + z, (x * q + last) * q + z
                lo, hi = ref[p], ref[r]
                ref[p] = jnp.where(first_y, lo, lo + shifted(hi, 1))
                ref[r] = jnp.where(last_y, hi, hi + shifted(lo, -1))

    def local_sum(ref, q, zs):
        sum_x(ref, q, zs, range(q))
        sum_y(ref, q, zs)

    def edge(dx, dy, q):
        xs = range(q) if dx == 0 else [0 if dx < 0 else q - 1]
        ys = range(q) if dy == 0 else [0 if dy < 0 else q - 1]
        planes = [(x * q + y) * q + z for x in xs for y in ys for z in range(q - 1)]
        e, f = (0 if dx < 0 else ex - 1), (0 if dy < 0 else ey - 1)
        if dy == 0:
            return planes, ey, slice(e * ey, (e + 1) * ey)
        if dx == 0:
            return planes, ex, pl.ds(f, ex, stride=ey)
        return planes, 1, slice(e * ey + f, e * ey + f + 1)

    def whole_rows(count):
        return -(-count // tile) * tile

    pending = []

    def start_exchange(level, stage, fields, ways=range(len(DIRS))):
        send, recv, sems = level
        copies = []
        for d in ways:
            dx, dy = DIRS[d]
            at = 0
            for ref, q in fields:
                planes, count, rows = edge(dx, dy, q)
                for p in planes:
                    send[stage, d, at : at + count, :] = ref[p, rows, :]
                    at += count
            total = whole_rows(at)
            copy = pltpu.make_async_remote_copy(
                src_ref=send.at[stage, d, pl.ds(0, total)],
                dst_ref=recv.at[stage, d, pl.ds(0, total)],
                send_sem=sems.at[0, stage, d],
                recv_sem=sems.at[1, stage, d],
                device_id=target(dx, dy),
                device_id_type=MESH,
            )
            copy.start()
            copies.append(copy)
        return copies

    def finish_exchange(level, stage, fields, copies, finals):
        _, recv, _ = level
        for d in reversed(range(len(DIRS))):
            dx, dy = DIRS[d]
            copies[d].wait_recv()
            at = 0
            for ref, q in fields:
                planes, count, rows = edge(-dx, -dy, q)
                for p in planes:
                    ref[p, rows, :] = ref[p, rows, :] + recv[stage, d, at : at + count, :]
                    at += count
        pending.extend(copies)
        for (ref, q), final in zip(fields, finals):
            for x in range(q):
                for y in range(q):
                    if x in (0, q - 1) or y in (0, q - 1):
                        p = (x * q + y) * q
                        for z in range(q - 1):
                            value = final(p + z, ref[p + z])
                            ref[p + z] = value
                            if z == 0:
                                ref[p + q - 1] = pltpu.roll(value, lanes - 1, 1)

    def interior(ref, q, final):
        for x in range(1, q - 1):
            for y in range(1, q - 1):
                for z in range(q):
                    p = (x * q + y) * q + z
                    ref[p] = final(p, ref[p])

    fine = (fine_send, fine_recv, fine_sems)
    rough = (coarse_send, coarse_recv, coarse_sems)

    def start_line(which, along_x, first, second):
        out, slots, sems = (
            (line_x_send, line_x, line_x_sem) if along_x else (line_y_send, line_y, line_y_sem)
        )
        count = nx if along_x else ny
        out[which, 0:1] = first
        out[which, 1:2] = second
        copies = []
        for o in range(1, count):
            copy = pltpu.make_async_remote_copy(
                src_ref=out.at[which],
                dst_ref=slots.at[which, o],
                send_sem=line_send_sem.at[which, 0 if along_x else 1, o],
                recv_sem=sems.at[which, o],
                device_id=target(o, 0) if along_x else target(0, o),
                device_id_type=MESH,
            )
            copy.start()
            copies.append(copy)
        return copies

    def finish_line(which, along_x, copies):
        out, slots = (line_x_send, line_x) if along_x else (line_y_send, line_y)
        count = nx if along_x else ny
        for copy in copies:
            copy.wait_recv()
        pending.extend(copies)
        total = out[which]
        for o in range(1, count):
            total = total + slots[which, o]
        return total[0:1], total[1:2]

    def inverse_estimate(first, second):
        first = jnp.sum(first, axis=1, keepdims=True)
        second = jnp.sum(second, axis=1, keepdims=True)
        return 1.0 / jnp.sqrt(second / (first + 1e-06))

    def coefficients(inv_est):
        power = inv_est
        out = []
        for c in CHEB:
            out.append(jnp.broadcast_to(c * power, (subs, lanes)))
            power = power * inv_est
        return out

    net = Lanes(QF, tile, ez)
    group = tile // ey

    def permuted(plane, index):
        tiles = [
            jnp.take_along_axis(plane[h * tile : (h + 1) * tile], index, axis=1)
            for h in range(subs // tile)
        ]
        return jnp.concatenate(tiles, axis=0)

    def read_planes(n, dst):
        for x in range(QF):
            for y in range(QF):
                for h in range(subs // tile):
                    blocks = []
                    for v in range(QF):
                        parts = [
                            stored[n, v, (h * group + e) * QF + x, pl.ds(y, ey, stride=QF), :]
                            for e in range(group)
                        ]
                        blocks.append(jnp.concatenate(parts, axis=0))
                    for z, block in enumerate(net.mix(blocks)):
                        dst[(x * QF + y) * QF + z, h * tile : (h + 1) * tile, :] = block

    (
        cflux,
        cmass,
        cinv,
        rload,
        cpow,
        cpow_2,
        rw0,
        rw1,
        rw2,
        crhs,
        cb,
        cw0,
        cw1,
        ccor,
    ) = [coarse.at[i] for i in range(14)]

    for copy in arriving[:QF]:
        copy.wait()
    read_planes(0, load)
    for z in range(QF):
        for x in range(QF):
            for y in range(QF):
                p = (x * QF + y) * QF + z
                load[p] = float(FINE_W[x] * FINE_W[y] * FINE_W[z]) * permuted(load[p], net.pick[z])
    for a in range(QF * QF):
        line = z_sum([load[a * QF], load[a * QF + QF - 1]], lanes)
        load[a * QF] = line[0]
        load[a * QF + QF - 1] = line[1]
    local_sum(load, QF, range(QF - 1))

    def each(q, body):
        @pl.loop(0, q * q)
        def _(a):
            for i in range(q):
                body(a * q + i)

    def squares(q, values):
        def body(a, acc):
            for i in range(q):
                v = values(a * q + i)
                acc = acc + v * v
            return acc

        total = lax.fori_loop(0, q * q, body, jnp.zeros((subs, lanes), jnp.float32))
        return jnp.sum(total, axis=0, keepdims=True)

    def store(dst, values):
        def body(p):
            dst[p] = values(p)

        return body

    def half_unless(mask):
        return jnp.where(mask, 1.0, 0.5)

    def weighted(line, ends):
        if ends is None:
            return line
        return [half_unless(ends[0]) * line[0]] + line[1:-1] + [half_unless(ends[1]) * line[-1]]

    def restrict(field, dst, summed):
        ends_x = (first_x, last_x) if summed else None
        ends_y = (first_y, last_y) if summed else None

        @pl.loop(0, QF)
        def _(a):
            for c in range(QF):
                line = [field[i * QF * QF + a * QF + c] for i in range(QF)]
                line = dense(TRANSFER, weighted(line, ends_x))
                for i in range(QC):
                    tmp_a[i * QF * QF + a * QF + c] = line[i]

        for a in range(QC):
            for c in range(QF):
                line = [tmp_a[a * QF * QF + i * QF + c] for i in range(QF)]
                line = dense(TRANSFER, weighted(line, ends_y))
                for i in range(QC):
                    tmp_b[a * QC * QF + i * QF + c] = line[i]

        for a in range(QC):
            for c in range(QC):
                line = dense(RESTRICT, [tmp_b[a * QC * QF + c * QF + i] for i in range(QF)])
                line = z_sum(line, lanes)
                for i in range(QC):
                    dst[a * QC * QC + c * QC + i] = line[i]

    def apply_fine(src, dst):
        local_op(src, dst, flux, mass, FINE_D, lanes)

    def apply_and_send(src, dst, stage):
        copies = []

        def first_part():
            sum_x(dst, QF, inner_f, (0, QF - 1))
            copies.extend(start_exchange(fine, stage, [(dst, QF)], range(6)))

        local_op(src, dst, flux, mass, FINE_D, lanes, first_part)
        sum_x(dst, QF, inner_f, range(1, QF - 1))
        sum_y(dst, QF, inner_f)
        return copies + start_exchange(fine, stage, [(dst, QF)], range(6, len(DIRS)))

    def apply_coarse(src, dst):
        local_op(src, dst, cflux, cmass, COARSE_D, lanes)

    keep = lambda p, v: v
    invert = lambda p, v: 1.0 / v
    scaled = lambda p, v: inv[p] * v
    cscaled = lambda p, v: cinv[p] * v
    inner_f, inner_c = range(QF - 1), range(QC - 1)

    pl.semaphore_wait(barrier, len(greeted))
    f_load = start_exchange(fine, 0, [(load, QF)])

    pick = {0: 0, 2: 1, 4: 2}
    for n, full, part in ((1, flux, cflux), (2, mass, cmass)):
        for copy in arriving[n * QF : (n + 1) * QF]:
            copy.wait()
        read_planes(n, full)
        for z in range(QF):
            for x in range(QF):
                for y in range(QF):
                    p = (x * QF + y) * QF + z
                    value = permuted(full[p], net.pick[z])
                    full[p] = float(FINE_W[x] * FINE_W[y] * FINE_W[z]) * value
                    if x in pick and y in pick and z in pick:
                        i, j, k = pick[x], pick[y], pick[z]
                        weight = float(COARSE_W[i] * COARSE_W[j] * COARSE_W[k])
                        part[(i * QC + j) * QC + k] = weight * value

    local_diag(inv, flux, mass, FINE_D, lanes)
    local_sum(inv, QF, inner_f)
    f_diag = start_exchange(fine, 1, [(inv, QF)])

    local_sum(load, QF, [QF - 1])
    restrict(load, rload, True)
    local_sum(rload, QC, inner_c)
    local_diag(cinv, cflux, cmass, COARSE_D, lanes)
    local_sum(cinv, QC, inner_c)
    c_0 = start_exchange(rough, 0, [(cinv, QC), (rload, QC)])
    interior(inv, QF, invert)

    finish_exchange(fine, 0, [(load, QF)], f_load, [keep])
    f_power = apply_and_send(load, power, 2)
    interior(power, QF, scaled)

    finish_exchange(fine, 1, [(inv, QF)], f_diag, [invert])
    each(QF, store(b0, lambda p: inv[p] * load[p]))
    f_w0 = apply_and_send(b0, b1, 3)

    local_sum(b1, QF, [QF - 1])
    restrict(b1, rw0, True)
    local_sum(rw0, QC, inner_c)
    interior(b1, QF, scaled)
    interior(cinv, QC, invert)
    finish_exchange(rough, 0, [(cinv, QC), (rload, QC)], c_0, [invert, keep])
    apply_coarse(rload, cpow)
    local_sum(cpow, QC, inner_c)
    c_1 = start_exchange(rough, 1, [(cpow, QC), (rw0, QC)])
    interior(cpow, QC, cscaled)

    finish_exchange(fine, 2, [(power, QF)], f_power, [scaled])
    f_power_2 = apply_and_send(power, power_2, 4)
    interior(power_2, QF, scaled)

    finish_exchange(fine, 3, [(b1, QF)], f_w0, [scaled])
    f_w1 = apply_and_send(b1, b2, 5)

    local_sum(b2, QF, [QF - 1])
    restrict(b2, rw1, True)
    local_sum(rw1, QC, inner_c)
    interior(b2, QF, scaled)
    finish_exchange(rough, 1, [(cpow, QC), (rw0, QC)], c_1, [cscaled, keep])
    apply_coarse(cpow, cpow_2)
    local_sum(cpow_2, QC, inner_c)
    c_2 = start_exchange(rough, 2, [(cpow_2, QC), (rw1, QC)])
    interior(cpow_2, QC, cscaled)
    sum_first = squares(QF, lambda p: power[p])

    finish_exchange(fine, 4, [(power_2, QF)], f_power_2, [scaled])
    sum_second = squares(QF, lambda p: power_2[p])
    line = start_line(0, True, sum_first, sum_second)

    finish_exchange(fine, 5, [(b2, QF)], f_w1, [scaled])
    line = start_line(0, False, *finish_line(0, True, line))
    apply_fine(b2, power)
    restrict(power, rw2, False)
    local_sum(rw2, QC, inner_c)
    c_3 = start_exchange(rough, 3, [(rw2, QC)])

    finish_exchange(rough, 2, [(cpow_2, QC), (rw1, QC)], c_2, [cscaled, keep])
    csum_first = squares(QC, lambda p: cpow[p])
    csum_second = squares(QC, lambda p: cpow_2[p])
    cline = start_line(1, True, csum_first, csum_second)
    scale = coefficients(inverse_estimate(*finish_line(0, False, line)))
    each(
        QF,
        store(smooth, lambda p: scale[0] * b0[p] + scale[1] * b1[p] + scale[2] * b2[p]),
    )
    each(QC, store(crhs, lambda p: rload[p] - (scale[0] * rw0[p] + scale[1] * rw1[p])))

    finish_exchange(rough, 3, [(rw2, QC)], c_3, [keep])
    each(QC, store(crhs, lambda p: crhs[p] - scale[2] * rw2[p]))
    each(QC, store(cb, lambda p: cinv[p] * crhs[p]))
    apply_coarse(cb, cw0)
    local_sum(cw0, QC, inner_c)
    c_4 = start_exchange(rough, 4, [(cw0, QC)])
    interior(cw0, QC, cscaled)
    cline = start_line(1, False, *finish_line(1, True, cline))

    finish_exchange(rough, 4, [(cw0, QC)], c_4, [cscaled])
    apply_coarse(cw0, cw1)
    local_sum(cw1, QC, inner_c)
    c_5 = start_exchange(rough, 5, [(cw1, QC)])
    interior(cw1, QC, cscaled)
    cscale = coefficients(inverse_estimate(*finish_line(1, False, cline)))
    each(QC, store(ccor, lambda p: cscale[0] * cb[p] + cscale[1] * cw0[p]))

    for copy in pending:
        copy.wait_send()
    pending.clear()

    finish_exchange(rough, 5, [(cw1, QC)], c_5, [cscaled])
    each(QC, store(ccor, lambda p: ccor[p] + cscale[2] * cw1[p]))

    def write_planes(dst, planes, q, lane_net):
        for x in range(q):
            for y in range(q):
                for h in range(subs // tile):
                    rows = slice(h * tile, (h + 1) * tile)
                    placed = [planes[(x * q + y) * q + z, rows, :] for z in range(q)]
                    for v, block in enumerate(lane_net.unmix(placed)):
                        for e in range(group):
                            part = block[e * ey : (e + 1) * ey]
                            dst[v, (h * group + e) * q + x, pl.ds(y, ey, stride=q), :] = part

    leaving = []
    cnet = Lanes(QC, tile, ez)
    for z in range(QC):
        for a in range(QC * QC):
            tmp_b[a * QC + z] = permuted(ccor[a * QC + z], cnet.place[z])
    write_planes(cresult, tmp_b, QC, cnet)
    for v in range(QC):
        copy = pltpu.make_async_copy(
            cresult.at[v], cor_hbm.at[:, :, v * ez : (v + 1) * ez], cor_sem.at[v]
        )
        copy.start()
        leaving.append(copy)
    for y in range(QC):
        for z in range(QC):
            line = dense(INTERP, [ccor[i * QC * QC + y * QC + z] for i in range(QC)])
            for i in range(QF):
                tmp_a[(i * QC + y) * QC + z] = line[i]
    for x in range(QF):
        for z in range(QC):
            line = dense(INTERP, [tmp_a[(x * QC + i) * QC + z] for i in range(QC)])
            for i in range(QF):
                tmp_b[(x * QF + i) * QC + z] = line[i]
    for z in range(QF):
        for a in range(QF * QF):
            p = a * QF + z
            lifted = dense(INTERP[z : z + 1], [tmp_b[a * QC + i] for i in range(QC)])[0]
            smooth[p] = permuted(smooth[p] + lifted, net.place[z])
    write_planes(result, smooth, QF, net)
    for v in range(QF):
        copy = pltpu.make_async_copy(
            result.at[v], out_hbm.at[:, :, v * ez : (v + 1) * ez], out_sem.at[v]
        )
        copy.start()
        leaving.append(copy)
    for copy in pending:
        copy.wait_send()
    for copy in leaving:
        copy.wait()


def hand_over(out_ref, cor_ref, out_hbm, cor_hbm, sems):
    copies = [
        pltpu.make_async_copy(out_ref, out_hbm, sems.at[0]),
        pltpu.make_async_copy(cor_ref, cor_hbm, sems.at[1]),
    ]
    for copy in copies:
        copy.start()
    for copy in copies:
        copy.wait()


def on_device(nx, ny, source, conductivity, absorption):
    px, py, pz = source.shape
    ex, ey, ez = px // QF, py // QF, pz // QF
    subs = ex * ey
    face = max(ex, ey)
    f32 = jnp.float32
    dirs = len(DIRS)
    longest = max(nx, ny)
    fine_rows = -(-QF * (QF - 1) * face // 8) * 8
    coarse_rows = -(-2 * QC * (QC - 1) * face // 8) * 8
    scratch = [
        pltpu.VMEM((3, QF, px, py, ez), f32),
        pltpu.VMEM((QF, px, py, ez), f32),
        pltpu.VMEM((QC, ex * QC, ey * QC, ez), f32),
        *[pltpu.VMEM((QF**3, subs, ez), f32)] * 10,
        pltpu.VMEM((14, QC**3, subs, ez), f32),
        pltpu.VMEM((QF * QF * QC, subs, ez), f32),
        pltpu.VMEM((QF * QF * QC, subs, ez), f32),
        *[pltpu.VMEM((FINE_STAGES, dirs, fine_rows, ez), f32)] * 2,
        *[pltpu.VMEM((COARSE_STAGES, dirs, coarse_rows, ez), f32)] * 2,
        pltpu.VMEM((2, 8, ez), f32),
        pltpu.VMEM((2, nx, 8, ez), f32),
        pltpu.VMEM((2, 8, ez), f32),
        pltpu.VMEM((2, ny, 8, ez), f32),
        pltpu.SemaphoreType.DMA((3, QF)),
        pltpu.SemaphoreType.DMA((QF,)),
        pltpu.SemaphoreType.DMA((QC,)),
        pltpu.SemaphoreType.DMA((2, FINE_STAGES, dirs)),
        pltpu.SemaphoreType.DMA((2, COARSE_STAGES, dirs)),
        pltpu.SemaphoreType.DMA((2, 2, longest)),
        pltpu.SemaphoreType.DMA((2, nx)),
        pltpu.SemaphoreType.DMA((2, ny)),
    ]
    anywhere = pl.BlockSpec(memory_space=pl.ANY)
    out, cor = pl.pallas_call(
        functools.partial(kernel, nx, ny),
        out_shape=(
            jax.ShapeDtypeStruct(source.shape, f32),
            jax.ShapeDtypeStruct((ex * QC, ey * QC, ez * QC), f32),
        ),
        in_specs=[pl.BlockSpec(memory_space=pltpu.HBM)] * 3,
        out_specs=(anywhere, anywhere),
        scratch_shapes=scratch,
        compiler_params=pltpu.CompilerParams(
            collective_id=0, has_side_effects=True, vmem_limit_bytes=52 * 1024 * 1024
        ),
    )(source, conductivity, absorption)
    return pl.pallas_call(
        hand_over,
        out_shape=(out, cor),
        in_specs=[anywhere] * 2,
        out_specs=(pl.BlockSpec(memory_space=pltpu.HBM),) * 2,
        scratch_shapes=[pltpu.SemaphoreType.DMA((2,))],
        compiler_params=pltpu.CompilerParams(vmem_limit_bytes=1024 * 1024),
    )(out, cor)


def solution(mesh):
    spec = P("gx", "gy", None)
    return jax.shard_map(
        functools.partial(on_device, mesh.shape["gx"], mesh.shape["gy"]),
        mesh=mesh,
        in_specs=(spec,) * 3,
        out_specs=(spec, spec),
        check_vma=False,
    )
```

```python
import functools
import math

import jax
import jax.numpy as jnp
import numpy as np
from jax import lax
from jax.experimental import pallas as pl
from jax.experimental.pallas import tpu as pltpu
from jax.sharding import PartitionSpec as P

SWEEPS = 3
MESH = pl.DeviceIdType.MESH
DIRS = [(-1, -1), (-1, 1), (1, -1), (1, 1), (0, -1), (0, 1), (-1, 0), (1, 0)]
FINE_STAGES, COARSE_STAGES = 6, 6


def deriv_table(points):
    count = len(points)
    barycentric = np.array(
        [
            1.0 / np.prod([points[j] - points[k] for k in range(count) if k != j])
            for j in range(count)
        ]
    )
    table = np.zeros((count, count))
    for i in range(count):
        for j in range(count):
            if i != j:
                table[i, j] = barycentric[j] / (barycentric[i] * (points[i] - points[j]))
        table[i, i] = -np.sum(table[i])
    return table


ROOT = math.sqrt(3.0 / 7.0)
FINE_POINTS = np.array([-1.0, -ROOT, 0.0, ROOT, 1.0])
FINE_W = np.array([0.1, 49.0 / 90.0, 32.0 / 45.0, 49.0 / 90.0, 0.1])
COARSE_POINTS = np.array([-1.0, 0.0, 1.0])
COARSE_W = np.array([1.0 / 3.0, 4.0 / 3.0, 1.0 / 3.0])
FINE_D = deriv_table(FINE_POINTS)
COARSE_D = deriv_table(COARSE_POINTS)
INTERP = np.stack(
    [
        FINE_POINTS * (FINE_POINTS - 1.0) / 2.0,
        1.0 - FINE_POINTS**2,
        FINE_POINTS * (FINE_POINTS + 1.0) / 2.0,
    ],
    1,
)
RESTRICT = INTERP.T * np.array([0.5, 1.0, 1.0, 1.0, 0.5])[None, :]
TRANSFER = INTERP.T
QF, QC = 5, 3


def chebyshev_coefficients():
    theta, delta, sigma, rho = 0.75, 0.45, 5.0 / 3.0, 0.6
    x = np.zeros(SWEEPS + 1)
    r = np.zeros(SWEEPS + 1)
    r[0] = 1.0
    d = r / theta
    for sweep in range(SWEEPS):
        x = x + d
        r = r - np.concatenate([[0.0], d[:-1]])
        if sweep + 1 < SWEEPS:
            rho_next = 1.0 / (2.0 * sigma - rho)
            d = rho_next * rho * d + 2.0 * rho_next / delta * r
            rho = rho_next
    return [float(v) for v in x[:SWEEPS]]


CHEB = chebyshev_coefficients()


def row_scales(table):
    n = table.shape[0]
    half = n // 2
    scale = np.ones(n)
    for i in range(half):
        scale[i] = scale[n - 1 - i] = 2.0 / (table[i, 0] + table[i, n - 1])
    scale[half] = 1.0 / table[half, 0]
    return scale


def halves(table):
    n = table.shape[0]
    half = n // 2
    scaled = row_scales(table)[:, None] * table
    even = [[(scaled[i, j] + scaled[i, n - 1 - j]) / 2 for j in range(half)] for i in range(half)]
    odd = [[(scaled[i, j] - scaled[i, n - 1 - j]) / 2 for j in range(half)] for i in range(half)]
    middle = [scaled[half, j] for j in range(half)]
    return even, odd, middle


def combine(weights, terms):
    acc = None
    for w, t in zip(weights, terms):
        w = float(w)
        if abs(w) < 1e-14:
            continue
        term = t if abs(w - 1.0) < 1e-12 else w * t
        acc = term if acc is None else acc + term
    return acc


def derive(table, u):
    n = len(u)
    half = n // 2
    even, odd, middle = halves(table)
    twice = u[half] + u[half]
    a = [u[j] + u[n - 1 - j] - twice for j in range(half)]
    o = [u[j] - u[n - 1 - j] for j in range(half)]
    out = [None] * n
    for i in range(half):
        p, q = combine(even[i], a), combine(odd[i], o)
        out[i], out[n - 1 - i] = q + p, q - p
    out[half] = combine(middle, o)
    return out


def derive_back(table, g):
    n = len(g)
    half = n // 2
    even, odd, middle = halves(table)
    plus = [g[i] + g[n - 1 - i] for i in range(half)]
    minus = [g[i] - g[n - 1 - i] for i in range(half)]
    out = [None] * n
    total = None
    for j in range(half):
        a = combine([even[i][j] for i in range(half)], minus)
        o = combine([odd[i][j] for i in range(half)] + [middle[j]], plus + [g[half]])
        out[j], out[n - 1 - j] = a + o, a - o
        total = a if total is None else total + a
    out[half] = -2.0 * total
    return out


def dense(table, u):
    out = []
    for i in range(table.shape[0]):
        acc = None
        for j in range(table.shape[1]):
            c = float(table[i, j])
            if abs(c) < 1e-14:
                continue
            term = u[j] if c == 1.0 else c * u[j]
            acc = term if acc is None else acc + term
        out.append(acc)
    return out


def centrosym(table, u):
    n = len(u)
    half = n // 2
    even = [u[j] + u[n - 1 - j] for j in range(half)]
    odd = [u[j] - u[n - 1 - j] for j in range(half)]
    out = [None] * n
    for i in range(half):
        s = [(table[i, j] + table[i, n - 1 - j]) / 2 for j in range(half)]
        t = [[(table[i, j] - table[i, n - 1 - j]) / 2 for j in range(half)]]
        p = dense(np.array([s + [table[i, half]]]), even + [u[half]])[0]
        q = dense(np.array(t), odd)[0]
        out[i] = p + q
        out[n - 1 - i] = p - q
    middle = np.array([[table[half, j] for j in range(half + 1)]])
    out[half] = dense(middle, even + [u[half]])[0]
    return out


def plane_starts(q, axis, a, b):
    strides = (q * q, q, 1)
    other = [s for k, s in enumerate(strides) if k != axis]
    return a * other[0] + b * other[1], strides[axis]


def z_sum(line, lanes):
    lo, hi = line[0], line[-1]
    line[-1] = hi + pltpu.roll(lo, lanes - 1, 1)
    line[0] = lo + pltpu.roll(hi, 1, 1)
    return line


def operator_lines(src, dst, flux, mass, table, lanes, axis, places):
    q = table.shape[0]

    def read(n):
        start, step = plane_starts(q, axis, *places[n])
        u = [src[start + step * i] for i in range(q)]
        base = None if axis == 0 else [dst[start + step * i] for i in range(q)]
        return u, base

    ahead = read(0)
    for n in range(len(places)):
        u, base = ahead
        if n + 1 < len(places):
            ahead = read(n + 1)
        start, step = plane_starts(q, axis, *places[n])
        g = derive(table, u)
        g = [flux[axis, start + step * i] * g[i] for i in range(q)]
        r = derive_back(table, g)
        for i in range(q):
            r[i] = (mass[start + step * i] * u[i] if base is None else base[i]) + r[i]
        if axis == 2:
            r = z_sum(r, lanes)
        for i in range(q):
            dst[start + step * i] = r[i]


def operator_start(src, dst, flux, mass, table, lanes):
    q = table.shape[0]

    @pl.loop(1, q - 1)
    def _(y):
        operator_lines(src, dst, flux, mass, table, lanes, 0, [(y, z) for z in range(q)])


def local_op(src, dst, flux, mass, table, lanes, between=None, started=False):
    q = table.shape[0]
    run = functools.partial(operator_lines, src, dst, flux, mass, table, lanes)
    if not started:
        operator_start(src, dst, flux, mass, table, lanes)
    run(0, [(y, z) for y in (0, q - 1) for z in range(q)])

    @pl.loop(0, q)
    def _(a):
        run(1, [(a, b) for b in range(q)])

    run(2, [(a, b) for b in (0, q - 1) for a in range(q)])
    if between is not None:
        between()
    run(2, [(a, b) for b in range(1, q - 1) for a in (0, q - 1)])
    run(2, [(a, b) for b in range(1, q - 1) for a in range(1, q - 1)])


def local_diag(dst, flux, mass, table, lanes):
    q = table.shape[0]
    square = (table * table).T

    def lines(axis, a):
        for b in range(q):
            start, step = plane_starts(q, axis, a, b)
            r = centrosym(square, [flux[start + step * i] for i in range(q)])
            for i in range(q):
                base = mass if axis == 0 else dst
                r[i] = base[start + step * i] + r[i]
            if axis == 2:
                r = z_sum(r, lanes)
            for i in range(q):
                dst[start + step * i] = r[i]

    for axis in range(2):

        @pl.loop(0, q)
        def _(a, axis=axis):
            lines(axis, a)

    for a in range(q):
        lines(2, a)


class Lanes:
    def __init__(self, q, rows, ez):
        self.q = q
        lane = lax.broadcasted_iota(jnp.int32, (rows, ez), 1)
        self.turn = ez % q
        self.back = pow(self.turn, -1, q)
        unit = pow(q, -1, ez)
        self.pick = [lax.rem(lane * q + k, ez) for k in range(q)]
        self.place = [lax.rem((lane + (ez - k)) * unit, ez) for k in range(q)]
        s = lax.rem(lane, q)
        self.out_steps = self.bits(s, q - self.back)
        self.in_steps = self.bits(s, self.back)

    def bits(self, s, by):
        amount = lax.rem(s * by, self.q)
        steps, step = [], 1
        while step < self.q:
            steps.append((step, lax.rem(lax.div(amount, step), 2) == 1))
            step *= 2
        return steps

    def select(self, blocks, steps):
        for step, mask in steps:
            blocks = [
                jnp.where(mask, blocks[(v + step) % self.q], blocks[v]) for v in range(self.q)
            ]
        return blocks

    def mix(self, blocks):
        mixed = self.select(blocks, self.out_steps)
        return [mixed[self.back * k % self.q] for k in range(self.q)]

    def unmix(self, placed):
        return self.select([placed[self.turn * j % self.q] for j in range(self.q)], self.in_steps)


def kernel(
    nx,
    ny,
    src_hbm,
    cond_hbm,
    abs_hbm,
    result,
    cresult,
    stored,
    load,
    inv,
    power,
    power_2,
    b0,
    b1,
    b2,
    flux,
    fluxes,
    cfluxes,
    mass,
    smooth,
    coarse,
    tmp_a,
    tmp_b,
    fine_send,
    fine_recv,
    coarse_send,
    coarse_recv,
    line_x_send,
    line_x,
    line_y_send,
    line_y,
    in_sem,
    fine_sems,
    coarse_sems,
    line_send_sem,
    line_x_sem,
    line_y_sem,
):
    px, py, pz = src_hbm.shape
    ex, ey, ez = px // QF, py // QF, pz // QF
    subs, lanes = ex * ey, ez
    tile = 8
    mx, my = lax.axis_index("gx"), lax.axis_index("gy")

    def target(dx, dy):
        return (lax.rem(mx + dx + nx, nx), lax.rem(my + dy + ny, ny))

    greeted = {(o, 0) for o in range(1, nx)} | {(0, o) for o in range(1, ny)}
    greeted |= {(dx % nx, dy % ny) for dx, dy in DIRS}
    greeted = sorted(greeted)
    barrier = pltpu.get_barrier_semaphore()
    for dx, dy in greeted:
        pl.semaphore_signal(barrier, inc=1, device_id=target(dx, dy), device_id_type=MESH)

    arriving = []
    for n, ref in enumerate((src_hbm, cond_hbm, abs_hbm)):
        for v in range(QF):
            copy = pltpu.make_async_copy(
                ref.at[:, :, v * ez : (v + 1) * ez], stored.at[n, v], in_sem.at[n, v]
            )
            copy.start()
            arriving.append(copy)

    sub = lax.broadcasted_iota(jnp.int32, (subs, lanes), 0)
    row_y = lax.rem(sub, ey)
    first_x, last_x = sub < ey, sub >= (ex - 1) * ey
    first_y, last_y = row_y == 0, row_y == ey - 1

    def shifted(plane, shift):
        return pltpu.roll(plane, shift % subs, 0)

    def sum_x(ref, q, zs, ys):
        last = q - 1
        for z in zs:
            for y in ys:
                p, r = y * q + z, (last * q + y) * q + z
                lo, hi = ref[p], ref[r]
                ref[p] = jnp.where(first_x, lo, lo + shifted(hi, ey))
                ref[r] = jnp.where(last_x, hi, hi + shifted(lo, -ey))

    def sum_y(ref, q, zs):
        last = q - 1
        for z in zs:
            for x in range(q):
                p, r = x * q * q + z, (x * q + last) * q + z
                lo, hi = ref[p], ref[r]
                ref[p] = jnp.where(first_y, lo, lo + shifted(hi, 1))
                ref[r] = jnp.where(last_y, hi, hi + shifted(lo, -1))

    def local_sum(ref, q, zs):
        sum_x(ref, q, zs, range(q))
        sum_y(ref, q, zs)

    def edge(dx, dy, q):
        xs = range(q) if dx == 0 else [0 if dx < 0 else q - 1]
        ys = range(q) if dy == 0 else [0 if dy < 0 else q - 1]
        planes = [(x * q + y) * q + z for x in xs for y in ys for z in range(q - 1)]
        e, f = (0 if dx < 0 else ex - 1), (0 if dy < 0 else ey - 1)
        if dy == 0:
            return planes, ey, slice(e * ey, (e + 1) * ey)
        if dx == 0:
            return planes, ex, pl.ds(f, ex, stride=ey)
        return planes, 1, slice(e * ey + f, e * ey + f + 1)

    def whole_rows(count):
        return -(-count // tile) * tile

    pending = []

    def start_exchange(level, stage, fields, ways=range(len(DIRS))):
        send, recv, sems = level
        copies = []
        for d in ways:
            dx, dy = DIRS[d]
            at = 0
            for ref, q in fields:
                planes, count, rows = edge(dx, dy, q)
                for p in planes:
                    send[stage, d, at : at + count, :] = ref[p, rows, :]
                    at += count
            total = whole_rows(at)
            copy = pltpu.make_async_remote_copy(
                src_ref=send.at[stage, d, pl.ds(0, total)],
                dst_ref=recv.at[stage, d, pl.ds(0, total)],
                send_sem=sems.at[0, stage, d],
                recv_sem=sems.at[1, stage, d],
                device_id=target(dx, dy),
                device_id_type=MESH,
            )
            copy.start()
            copies.append(copy)
        return copies

    def finish_exchange(level, stage, fields, copies, finals, meanwhile=None):
        _, recv, _ = level
        for d in reversed(range(len(DIRS))):
            dx, dy = DIRS[d]
            copies[d].wait_recv()
            at = 0
            for ref, q in fields:
                planes, count, rows = edge(-dx, -dy, q)
                for p in planes:
                    ref[p, rows, :] = ref[p, rows, :] + recv[stage, d, at : at + count, :]
                    at += count
            if d == len(DIRS) - 2:
                for (ref, q), final in zip(fields, finals):
                    boundary(ref, ref, q, final, range(1, q - 1))
                if meanwhile is not None:
                    meanwhile()
        pending.extend(copies)
        for (ref, q), final in zip(fields, finals):
            boundary(ref, ref, q, final, (0, q - 1))

    def boundary(ref, dst, q, final, ys):
        for x in range(q):
            for y in ys:
                if x in (0, q - 1) or y in (0, q - 1):
                    p = (x * q + y) * q
                    for z in range(q - 1):
                        value = final(p + z, ref[p + z])
                        dst[p + z] = value
                        if z == 0:
                            dst[p + q - 1] = pltpu.roll(value, lanes - 1, 1)

    def interior(ref, q, final, dst=None):
        dst = ref if dst is None else dst
        for x in range(1, q - 1):
            for y in range(1, q - 1):
                for z in range(q):
                    p = (x * q + y) * q + z
                    dst[p] = final(p, ref[p])

    fine = (fine_send, fine_recv, fine_sems)
    rough = (coarse_send, coarse_recv, coarse_sems)

    def start_line(which, along_x, first, second):
        out, slots, sems = (
            (line_x_send, line_x, line_x_sem) if along_x else (line_y_send, line_y, line_y_sem)
        )
        count = nx if along_x else ny
        out[which, 0:1] = first
        out[which, 1:2] = second
        copies = []
        for o in range(1, count):
            copy = pltpu.make_async_remote_copy(
                src_ref=out.at[which],
                dst_ref=slots.at[which, o],
                send_sem=line_send_sem.at[which, 0 if along_x else 1, o],
                recv_sem=sems.at[which, o],
                device_id=target(o, 0) if along_x else target(0, o),
                device_id_type=MESH,
            )
            copy.start()
            copies.append(copy)
        return copies

    def finish_line(which, along_x, copies):
        out, slots = (line_x_send, line_x) if along_x else (line_y_send, line_y)
        count = nx if along_x else ny
        for copy in copies:
            copy.wait_recv()
        pending.extend(copies)
        total = out[which]
        for o in range(1, count):
            total = total + slots[which, o]
        return total[0:1], total[1:2]

    def inverse_estimate(first, second):
        first = jnp.sum(first, axis=1, keepdims=True)
        second = jnp.sum(second, axis=1, keepdims=True)
        return 1.0 / jnp.sqrt(second / (first + 1e-06))

    def coefficients(inv_est):
        power = inv_est
        out = []
        for c in CHEB:
            out.append(jnp.broadcast_to(c * power, (subs, lanes)))
            power = power * inv_est
        return out

    net = Lanes(QF, tile, ez)
    group = tile // ey

    def permuted(plane, index):
        tiles = [
            jnp.take_along_axis(plane[h * tile : (h + 1) * tile], index, axis=1)
            for h in range(subs // tile)
        ]
        return jnp.concatenate(tiles, axis=0)

    def read_planes(n, dst):
        for x in range(QF):
            for y in range(QF):
                for h in range(subs // tile):
                    blocks = []
                    for v in range(QF):
                        parts = [
                            stored[n, v, (h * group + e) * QF + x, pl.ds(y, ey, stride=QF), :]
                            for e in range(group)
                        ]
                        blocks.append(jnp.concatenate(parts, axis=0))
                    for z, block in enumerate(net.mix(blocks)):
                        dst[(x * QF + y) * QF + z, h * tile : (h + 1) * tile, :] = block

    (
        cflux,
        cmass,
        cinv,
        rload,
        cpow,
        cpow_2,
        rw0,
        rw1,
        rw2,
        crhs,
        cw0,
        cw1,
        ccor,
    ) = [coarse.at[i] for i in range(13)]

    for copy in arriving[:QF]:
        copy.wait()
    read_planes(0, load)
    for z in range(QF):
        for x in range(QF):
            for y in range(QF):
                p = (x * QF + y) * QF + z
                load[p] = float(FINE_W[x] * FINE_W[y] * FINE_W[z]) * permuted(load[p], net.pick[z])
    for a in range(QF * QF):
        line = z_sum([load[a * QF], load[a * QF + QF - 1]], lanes)
        load[a * QF] = line[0]
        load[a * QF + QF - 1] = line[1]
    local_sum(load, QF, range(QF - 1))

    def each(q, body):
        @pl.loop(0, q * q)
        def _(a):
            for i in range(q):
                body(a * q + i)

    def squares(q, values):
        def body(a, acc):
            for i in range(q):
                v = values(a * q + i)
                acc = acc + v * v
            return acc

        total = lax.fori_loop(0, q * q, body, jnp.zeros((subs, lanes), jnp.float32))
        return jnp.sum(total, axis=0, keepdims=True)

    def store(dst, values):
        def body(p):
            dst[p] = values(p)

        return body

    def half_unless(mask):
        return jnp.where(mask, 1.0, 0.5)

    def weighted(line, ends):
        if ends is None:
            return line
        return [half_unless(ends[0]) * line[0]] + line[1:-1] + [half_unless(ends[1]) * line[-1]]

    def restrict(field, dst, summed):
        ends_x = (first_x, last_x) if summed else None
        ends_y = (first_y, last_y) if summed else None

        @pl.loop(0, QF)
        def _(a):
            for c in range(QF):
                line = [field[i * QF * QF + a * QF + c] for i in range(QF)]
                line = dense(TRANSFER, weighted(line, ends_x))
                for i in range(QC):
                    tmp_a[i * QF * QF + a * QF + c] = line[i]

        for a in range(QC):
            for c in range(QF):
                line = [tmp_a[a * QF * QF + i * QF + c] for i in range(QF)]
                line = dense(TRANSFER, weighted(line, ends_y))
                for i in range(QC):
                    tmp_b[a * QC * QF + i * QF + c] = line[i]

        for a in range(QC):
            for c in range(QC):
                line = dense(RESTRICT, [tmp_b[a * QC * QF + c * QF + i] for i in range(QF)])
                line = z_sum(line, lanes)
                for i in range(QC):
                    dst[a * QC * QC + c * QC + i] = line[i]

    def scaled_fluxes(flux, scaled, table):
        q = table.shape[0]
        square = 1.0 / row_scales(table) ** 2

        for x in range(q):
            for y in range(q):
                for z in range(q):
                    p = (x * q + y) * q + z
                    value = flux[p]
                    for axis, i in enumerate((x, y, z)):
                        scaled[axis, p] = float(square[i]) * value

    def start_apply(src, dst):
        return lambda: operator_start(src, dst, fluxes, mass, FINE_D, lanes)

    def apply_and_send(src, dst, stage, started=True):
        copies = []

        def first_part():
            sum_x(dst, QF, inner_f, (0, QF - 1))
            copies.extend(start_exchange(fine, stage, [(dst, QF)], range(6)))

        local_op(src, dst, fluxes, mass, FINE_D, lanes, first_part, started)
        sum_x(dst, QF, inner_f, range(1, QF - 1))
        sum_y(dst, QF, inner_f)
        return copies + start_exchange(fine, stage, [(dst, QF)], range(6, len(DIRS)))

    def apply_coarse(src, dst):
        local_op(src, dst, cfluxes, cmass, COARSE_D, lanes)

    keep = lambda p, v: v
    invert = lambda p, v: 1.0 / v
    scaled = lambda p, v: inv[p] * v
    cscaled = lambda p, v: cinv[p] * v
    inner_f, inner_c = range(QF - 1), range(QC - 1)

    pl.semaphore_wait(barrier, len(greeted))
    f_load = start_exchange(fine, 0, [(load, QF)])

    pick = {0: 0, 2: 1, 4: 2}
    for n, full, part in ((1, flux, cflux), (2, mass, cmass)):
        for copy in arriving[n * QF : (n + 1) * QF]:
            copy.wait()
        read_planes(n, full)
        for z in range(QF):
            for x in range(QF):
                for y in range(QF):
                    p = (x * QF + y) * QF + z
                    value = permuted(full[p], net.pick[z])
                    full[p] = float(FINE_W[x] * FINE_W[y] * FINE_W[z]) * value
                    if x in pick and y in pick and z in pick:
                        i, j, k = pick[x], pick[y], pick[z]
                        weight = float(COARSE_W[i] * COARSE_W[j] * COARSE_W[k])
                        part[(i * QC + j) * QC + k] = weight * value

    local_diag(inv, flux, mass, FINE_D, lanes)
    local_sum(inv, QF, inner_f)
    f_diag = start_exchange(fine, 1, [(inv, QF)])

    local_sum(load, QF, [QF - 1])
    restrict(load, rload, True)
    local_sum(rload, QC, inner_c)
    local_diag(cinv, cflux, cmass, COARSE_D, lanes)
    local_sum(cinv, QC, inner_c)
    c_0 = start_exchange(rough, 0, [(cinv, QC), (rload, QC)])
    scaled_fluxes(flux, fluxes, FINE_D)
    scaled_fluxes(cflux, cfluxes, COARSE_D)
    interior(inv, QF, invert)

    finish_exchange(fine, 0, [(load, QF)], f_load, [keep], start_apply(load, power))
    f_power = apply_and_send(load, power, 2)
    interior(power, QF, scaled)

    interior(load, QF, scaled, b0)

    def start_b0():
        boundary(load, b0, QF, scaled, range(1, QF - 1))
        operator_start(b0, b1, fluxes, mass, FINE_D, lanes)

    finish_exchange(fine, 1, [(inv, QF)], f_diag, [invert], start_b0)
    boundary(load, b0, QF, scaled, (0, QF - 1))
    f_w0 = apply_and_send(b0, b1, 3)

    local_sum(b1, QF, [QF - 1])
    restrict(b1, rw0, True)
    local_sum(rw0, QC, inner_c)
    interior(b1, QF, scaled)
    interior(cinv, QC, invert)
    finish_exchange(rough, 0, [(cinv, QC), (rload, QC)], c_0, [invert, keep])
    apply_coarse(rload, cpow)
    local_sum(cpow, QC, inner_c)
    c_1 = start_exchange(rough, 1, [(cpow, QC), (rw0, QC)])
    interior(cpow, QC, cscaled)

    finish_exchange(fine, 2, [(power, QF)], f_power, [scaled], start_apply(power, power_2))
    f_power_2 = apply_and_send(power, power_2, 4)
    interior(power_2, QF, scaled)

    finish_exchange(fine, 3, [(b1, QF)], f_w0, [scaled], start_apply(b1, b2))
    f_w1 = apply_and_send(b1, b2, 5)

    local_sum(b2, QF, [QF - 1])
    restrict(b2, rw1, True)
    local_sum(rw1, QC, inner_c)
    interior(b2, QF, scaled)
    finish_exchange(rough, 1, [(cpow, QC), (rw0, QC)], c_1, [cscaled, keep])
    apply_coarse(cpow, cpow_2)
    local_sum(cpow_2, QC, inner_c)
    c_2 = start_exchange(rough, 2, [(cpow_2, QC), (rw1, QC)])
    interior(cpow_2, QC, cscaled)
    sum_first = squares(QF, lambda p: power[p])

    finish_exchange(fine, 4, [(power_2, QF)], f_power_2, [scaled])
    sum_second = squares(QF, lambda p: power_2[p])
    line = start_line(0, True, sum_first, sum_second)

    finish_exchange(fine, 5, [(b2, QF)], f_w1, [scaled], start_apply(b2, power))
    across = []

    def forward():
        across.extend(start_line(0, False, *finish_line(0, True, line)))

    local_op(b2, power, fluxes, mass, FINE_D, lanes, forward, True)
    restrict(power, rw2, False)
    local_sum(rw2, QC, inner_c)
    c_3 = start_exchange(rough, 3, [(rw2, QC)])

    finish_exchange(rough, 2, [(cpow_2, QC), (rw1, QC)], c_2, [cscaled, keep])
    csum_first = squares(QC, lambda p: cpow[p])
    csum_second = squares(QC, lambda p: cpow_2[p])
    cline = start_line(1, True, csum_first, csum_second)
    scale = coefficients(inverse_estimate(*finish_line(0, False, across)))
    each(
        QF,
        store(smooth, lambda p: scale[0] * b0[p] + scale[1] * b1[p] + scale[2] * b2[p]),
    )
    each(QC, store(crhs, lambda p: rload[p] - (scale[0] * rw0[p] + scale[1] * rw1[p])))

    first = lambda p, v: cinv[p] * (crhs[p] - scale[2] * v)
    interior(rw2, QC, first)
    finish_exchange(rough, 3, [(rw2, QC)], c_3, [first])
    apply_coarse(rw2, cw0)
    local_sum(cw0, QC, inner_c)
    c_4 = start_exchange(rough, 4, [(cw0, QC)])
    interior(cw0, QC, cscaled)
    cline = start_line(1, False, *finish_line(1, True, cline))

    finish_exchange(rough, 4, [(cw0, QC)], c_4, [cscaled])
    apply_coarse(cw0, cw1)
    local_sum(cw1, QC, inner_c)
    c_5 = start_exchange(rough, 5, [(cw1, QC)])
    interior(cw1, QC, cscaled)
    cscale = coefficients(inverse_estimate(*finish_line(1, False, cline)))
    each(QC, store(ccor, lambda p: cscale[0] * rw2[p] + cscale[1] * cw0[p]))

    for copy in pending:
        copy.wait_send()
    pending.clear()

    finish_exchange(rough, 5, [(cw1, QC)], c_5, [cscaled])
    each(QC, store(ccor, lambda p: ccor[p] + cscale[2] * cw1[p]))

    def write_planes(dst, planes, q, lane_net):
        for x in range(q):
            for y in range(q):
                for h in range(subs // tile):
                    rows = slice(h * tile, (h + 1) * tile)
                    placed = [planes[(x * q + y) * q + z, rows, :] for z in range(q)]
                    for v, block in enumerate(lane_net.unmix(placed)):
                        for e in range(group):
                            part = block[e * ey : (e + 1) * ey]
                            dst[v, (h * group + e) * q + x, pl.ds(y, ey, stride=q), :] = part

    cnet = Lanes(QC, tile, ez)
    for z in range(QC):
        for a in range(QC * QC):
            tmp_b[a * QC + z] = permuted(ccor[a * QC + z], cnet.place[z])
    write_planes(cresult, tmp_b, QC, cnet)
    for y in range(QC):
        for z in range(QC):
            line = dense(INTERP, [ccor[i * QC * QC + y * QC + z] for i in range(QC)])
            for i in range(QF):
                tmp_a[(i * QC + y) * QC + z] = line[i]
    for x in range(QF):
        for z in range(QC):
            line = dense(INTERP, [tmp_a[(x * QC + i) * QC + z] for i in range(QC)])
            for i in range(QF):
                tmp_b[(x * QF + i) * QC + z] = line[i]
    for z in range(QF):
        for a in range(QF * QF):
            p = a * QF + z
            lifted = dense(INTERP[z : z + 1], [tmp_b[a * QC + i] for i in range(QC)])[0]
            smooth[p] = permuted(smooth[p] + lifted, net.place[z])
    write_planes(result, smooth, QF, net)
    for copy in pending:
        copy.wait_send()


def hand_over(result, cresult, out_hbm, cor_hbm, out_sem, cor_sem):
    copies = []
    for blocks, whole, sems in ((result, out_hbm, out_sem), (cresult, cor_hbm, cor_sem)):
        count, _, _, ez = blocks.shape
        for v in range(count):
            lanes = whole.at[:, :, v * ez : (v + 1) * ez]
            copies.append(pltpu.make_async_copy(blocks.at[v], lanes, sems.at[v]))
    for copy in copies:
        copy.start()
    for copy in copies:
        copy.wait()


def on_device(nx, ny, source, conductivity, absorption):
    px, py, pz = source.shape
    ex, ey, ez = px // QF, py // QF, pz // QF
    subs = ex * ey
    face = max(ex, ey)
    f32 = jnp.float32
    dirs = len(DIRS)
    longest = max(nx, ny)
    fine_rows = -(-QF * (QF - 1) * face // 8) * 8
    coarse_rows = -(-2 * QC * (QC - 1) * face // 8) * 8
    scratch = [
        pltpu.VMEM((3, QF, px, py, ez), f32),
        *[pltpu.VMEM((QF**3, subs, ez), f32)] * 8,
        pltpu.VMEM((3, QF**3, subs, ez), f32),
        pltpu.VMEM((3, QC**3, subs, ez), f32),
        *[pltpu.VMEM((QF**3, subs, ez), f32)] * 2,
        pltpu.VMEM((13, QC**3, subs, ez), f32),
        pltpu.VMEM((QF * QF * QC, subs, ez), f32),
        pltpu.VMEM((QF * QF * QC, subs, ez), f32),
        *[pltpu.VMEM((FINE_STAGES, dirs, fine_rows, ez), f32)] * 2,
        *[pltpu.VMEM((COARSE_STAGES, dirs, coarse_rows, ez), f32)] * 2,
        pltpu.VMEM((2, 8, ez), f32),
        pltpu.VMEM((2, nx, 8, ez), f32),
        pltpu.VMEM((2, 8, ez), f32),
        pltpu.VMEM((2, ny, 8, ez), f32),
        pltpu.SemaphoreType.DMA((3, QF)),
        pltpu.SemaphoreType.DMA((2, FINE_STAGES, dirs)),
        pltpu.SemaphoreType.DMA((2, COARSE_STAGES, dirs)),
        pltpu.SemaphoreType.DMA((2, 2, longest)),
        pltpu.SemaphoreType.DMA((2, nx)),
        pltpu.SemaphoreType.DMA((2, ny)),
    ]
    anywhere = pl.BlockSpec(memory_space=pl.ANY)
    out, cor = pl.pallas_call(
        functools.partial(kernel, nx, ny),
        out_shape=(
            jax.ShapeDtypeStruct((QF, px, py, ez), f32),
            jax.ShapeDtypeStruct((QC, ex * QC, ey * QC, ez), f32),
        ),
        in_specs=[pl.BlockSpec(memory_space=pltpu.HBM)] * 3,
        out_specs=(pl.BlockSpec(memory_space=pltpu.VMEM),) * 2,
        scratch_shapes=scratch,
        compiler_params=pltpu.CompilerParams(
            collective_id=0, has_side_effects=True, vmem_limit_bytes=52 * 1024 * 1024
        ),
    )(source, conductivity, absorption)
    return pl.pallas_call(
        hand_over,
        out_shape=(
            jax.ShapeDtypeStruct(source.shape, f32),
            jax.ShapeDtypeStruct((ex * QC, ey * QC, ez * QC), f32),
        ),
        in_specs=[anywhere] * 2,
        out_specs=(pl.BlockSpec(memory_space=pltpu.HBM),) * 2,
        scratch_shapes=[pltpu.SemaphoreType.DMA((QF,)), pltpu.SemaphoreType.DMA((QC,))],
        compiler_params=pltpu.CompilerParams(vmem_limit_bytes=1024 * 1024),
    )(out, cor)


def solution(mesh):
    spec = P("gx", "gy", None)
    return jax.shard_map(
        functools.partial(on_device, mesh.shape["gx"], mesh.shape["gy"]),
        mesh=mesh,
        in_specs=(spec,) * 3,
        out_specs=(spec, spec),
        check_vma=False,
    )
```

```python
import functools
import math

import jax
import jax.numpy as jnp
import numpy as np
from jax import lax
from jax.experimental import pallas as pl
from jax.experimental.pallas import tpu as pltpu
from jax.sharding import PartitionSpec as P

SWEEPS = 3
MESH = pl.DeviceIdType.MESH
DIRS = [(-1, -1), (-1, 1), (1, -1), (1, 1), (0, -1), (0, 1), (-1, 0), (1, 0)]
FINE_STAGES, COARSE_STAGES = 6, 6


def deriv_table(points):
    count = len(points)
    barycentric = np.array(
        [
            1.0 / np.prod([points[j] - points[k] for k in range(count) if k != j])
            for j in range(count)
        ]
    )
    table = np.zeros((count, count))
    for i in range(count):
        for j in range(count):
            if i != j:
                table[i, j] = barycentric[j] / (barycentric[i] * (points[i] - points[j]))
        table[i, i] = -np.sum(table[i])
    return table


ROOT = math.sqrt(3.0 / 7.0)
FINE_POINTS = np.array([-1.0, -ROOT, 0.0, ROOT, 1.0])
FINE_W = np.array([0.1, 49.0 / 90.0, 32.0 / 45.0, 49.0 / 90.0, 0.1])
COARSE_POINTS = np.array([-1.0, 0.0, 1.0])
COARSE_W = np.array([1.0 / 3.0, 4.0 / 3.0, 1.0 / 3.0])
FINE_D = deriv_table(FINE_POINTS)
COARSE_D = deriv_table(COARSE_POINTS)
INTERP = np.stack(
    [
        FINE_POINTS * (FINE_POINTS - 1.0) / 2.0,
        1.0 - FINE_POINTS**2,
        FINE_POINTS * (FINE_POINTS + 1.0) / 2.0,
    ],
    1,
)
RESTRICT = INTERP.T * np.array([0.5, 1.0, 1.0, 1.0, 0.5])[None, :]
TRANSFER = INTERP.T
QF, QC = 5, 3


def chebyshev_coefficients():
    theta, delta, sigma, rho = 0.75, 0.45, 5.0 / 3.0, 0.6
    x = np.zeros(SWEEPS + 1)
    r = np.zeros(SWEEPS + 1)
    r[0] = 1.0
    d = r / theta
    for sweep in range(SWEEPS):
        x = x + d
        r = r - np.concatenate([[0.0], d[:-1]])
        if sweep + 1 < SWEEPS:
            rho_next = 1.0 / (2.0 * sigma - rho)
            d = rho_next * rho * d + 2.0 * rho_next / delta * r
            rho = rho_next
    return [float(v) for v in x[:SWEEPS]]


CHEB = chebyshev_coefficients()


def row_scales(table):
    n = table.shape[0]
    half = n // 2
    scale = np.ones(n)
    for i in range(half):
        scale[i] = scale[n - 1 - i] = 2.0 / (table[i, 0] + table[i, n - 1])
    scale[half] = 1.0 / table[half, 0]
    return scale


def halves(table):
    n = table.shape[0]
    half = n // 2
    scaled = row_scales(table)[:, None] * table
    even = [[(scaled[i, j] + scaled[i, n - 1 - j]) / 2 for j in range(half)] for i in range(half)]
    odd = [[(scaled[i, j] - scaled[i, n - 1 - j]) / 2 for j in range(half)] for i in range(half)]
    middle = [scaled[half, j] for j in range(half)]
    return even, odd, middle


def combine(weights, terms):
    acc = None
    for w, t in zip(weights, terms):
        w = float(w)
        if abs(w) < 1e-14:
            continue
        term = t if abs(w - 1.0) < 1e-12 else w * t
        acc = term if acc is None else acc + term
    return acc


def derive(table, u):
    n = len(u)
    half = n // 2
    even, odd, middle = halves(table)
    twice = u[half] + u[half]
    a = [u[j] + u[n - 1 - j] - twice for j in range(half)]
    o = [u[j] - u[n - 1 - j] for j in range(half)]
    out = [None] * n
    for i in range(half):
        p, q = combine(even[i], a), combine(odd[i], o)
        out[i], out[n - 1 - i] = q + p, q - p
    out[half] = combine(middle, o)
    return out


def derive_back(table, g):
    n = len(g)
    half = n // 2
    even, odd, middle = halves(table)
    plus = [g[i] + g[n - 1 - i] for i in range(half)]
    minus = [g[i] - g[n - 1 - i] for i in range(half)]
    out = [None] * n
    total = None
    for j in range(half):
        a = combine([even[i][j] for i in range(half)], minus)
        o = combine([odd[i][j] for i in range(half)] + [middle[j]], plus + [g[half]])
        out[j], out[n - 1 - j] = a + o, a - o
        total = a if total is None else total + a
    out[half] = -2.0 * total
    return out


def dense(table, u):
    out = []
    for i in range(table.shape[0]):
        acc = None
        for j in range(table.shape[1]):
            c = float(table[i, j])
            if abs(c) < 1e-14:
                continue
            term = u[j] if c == 1.0 else c * u[j]
            acc = term if acc is None else acc + term
        out.append(acc)
    return out


def centrosym(table, u):
    n = len(u)
    half = n // 2
    even = [u[j] + u[n - 1 - j] for j in range(half)]
    odd = [u[j] - u[n - 1 - j] for j in range(half)]
    out = [None] * n
    for i in range(half):
        s = [(table[i, j] + table[i, n - 1 - j]) / 2 for j in range(half)]
        t = [[(table[i, j] - table[i, n - 1 - j]) / 2 for j in range(half)]]
        p = dense(np.array([s + [table[i, half]]]), even + [u[half]])[0]
        q = dense(np.array(t), odd)[0]
        out[i] = p + q
        out[n - 1 - i] = p - q
    middle = np.array([[table[half, j] for j in range(half + 1)]])
    out[half] = dense(middle, even + [u[half]])[0]
    return out


def plane_starts(q, axis, a, b):
    strides = (q * q, q, 1)
    other = [s for k, s in enumerate(strides) if k != axis]
    return a * other[0] + b * other[1], strides[axis]


def z_sum(line, lanes):
    lo, hi = line[0], line[-1]
    line[-1] = hi + pltpu.roll(lo, lanes - 1, 1)
    line[0] = lo + pltpu.roll(hi, 1, 1)
    return line


def operator_lines(src, dst, flux, mass, table, lanes, axis, places):
    q = table.shape[0]

    def read(n):
        start, step = plane_starts(q, axis, *places[n])
        u = [src[start + step * i] for i in range(q)]
        base = None if axis == 0 else [dst[start + step * i] for i in range(q)]
        return u, base

    ahead = read(0)
    for n in range(len(places)):
        u, base = ahead
        if n + 1 < len(places):
            ahead = read(n + 1)
        start, step = plane_starts(q, axis, *places[n])
        g = derive(table, u)
        g = [flux[axis, start + step * i] * g[i] for i in range(q)]
        r = derive_back(table, g)
        for i in range(q):
            r[i] = (mass[start + step * i] * u[i] if base is None else base[i]) + r[i]
        if axis == 2:
            r = z_sum(r, lanes)
        for i in range(q):
            dst[start + step * i] = r[i]


def operator_start(src, dst, flux, mass, table, lanes):
    q = table.shape[0]

    @pl.loop(1, q - 1)
    def _(y):
        operator_lines(src, dst, flux, mass, table, lanes, 0, [(y, z) for z in range(q)])


def local_op(src, dst, flux, mass, table, lanes, between=None, started=False):
    q = table.shape[0]
    run = functools.partial(operator_lines, src, dst, flux, mass, table, lanes)
    if not started:
        operator_start(src, dst, flux, mass, table, lanes)
    run(0, [(y, z) for y in (0, q - 1) for z in range(q)])

    @pl.loop(0, q)
    def _(a):
        run(1, [(a, b) for b in range(q)])

    run(2, [(a, b) for b in (0, q - 1) for a in range(q)])
    if between is not None:
        between()
    run(2, [(a, b) for b in range(1, q - 1) for a in (0, q - 1)])
    run(2, [(a, b) for b in range(1, q - 1) for a in range(1, q - 1)])


def local_diag(dst, flux, mass, table, lanes):
    q = table.shape[0]
    square = (table * table).T

    def lines(axis, a):
        for b in range(q):
            start, step = plane_starts(q, axis, a, b)
            r = centrosym(square, [flux[start + step * i] for i in range(q)])
            for i in range(q):
                base = mass if axis == 0 else dst
                r[i] = base[start + step * i] + r[i]
            if axis == 2:
                r = z_sum(r, lanes)
            for i in range(q):
                dst[start + step * i] = r[i]

    for axis in range(2):

        @pl.loop(0, q)
        def _(a, axis=axis):
            lines(axis, a)

    for a in range(q):
        lines(2, a)


class Lanes:
    def __init__(self, q, rows, ez):
        self.q = q
        lane = lax.broadcasted_iota(jnp.int32, (rows, ez), 1)
        self.turn = ez % q
        self.back = pow(self.turn, -1, q)
        unit = pow(q, -1, ez)
        self.pick = [lax.rem(lane * q + k, ez) for k in range(q)]
        self.place = [lax.rem((lane + (ez - k)) * unit, ez) for k in range(q)]
        s = lax.rem(lane, q)
        self.out_steps = self.bits(s, q - self.back)
        self.in_steps = self.bits(s, self.back)

    def bits(self, s, by):
        amount = lax.rem(s * by, self.q)
        steps, step = [], 1
        while step < self.q:
            steps.append((step, lax.rem(lax.div(amount, step), 2) == 1))
            step *= 2
        return steps

    def select(self, blocks, steps):
        for step, mask in steps:
            blocks = [
                jnp.where(mask, blocks[(v + step) % self.q], blocks[v]) for v in range(self.q)
            ]
        return blocks

    def mix(self, blocks):
        mixed = self.select(blocks, self.out_steps)
        return [mixed[self.back * k % self.q] for k in range(self.q)]

    def unmix(self, placed):
        return self.select([placed[self.turn * j % self.q] for j in range(self.q)], self.in_steps)


def kernel(
    nx,
    ny,
    src_hbm,
    cond_hbm,
    abs_hbm,
    result,
    cresult,
    stored,
    load,
    inv,
    power,
    power_2,
    b0,
    b1,
    b2,
    flux,
    fluxes,
    cfluxes,
    mass,
    smooth,
    coarse,
    tmp_a,
    tmp_b,
    fine_send,
    fine_recv,
    coarse_send,
    coarse_recv,
    line_x_send,
    line_x,
    line_y_send,
    line_y,
    in_sem,
    fine_sems,
    coarse_sems,
    line_send_sem,
    line_x_sem,
    line_y_sem,
):
    px, py, pz = src_hbm.shape
    ex, ey, ez = px // QF, py // QF, pz // QF
    subs, lanes = ex * ey, ez
    tile = 8
    mx, my = lax.axis_index("gx"), lax.axis_index("gy")

    def target(dx, dy):
        return (lax.rem(mx + dx + nx, nx), lax.rem(my + dy + ny, ny))

    greeted = {(o, 0) for o in range(1, nx)} | {(0, o) for o in range(1, ny)}
    greeted |= {(dx % nx, dy % ny) for dx, dy in DIRS}
    greeted = sorted(greeted)
    barrier = pltpu.get_barrier_semaphore()
    for dx, dy in greeted:
        pl.semaphore_signal(barrier, inc=1, device_id=target(dx, dy), device_id_type=MESH)

    arriving = []
    for n, ref in enumerate((src_hbm, cond_hbm, abs_hbm)):
        for v in range(QF):
            copy = pltpu.make_async_copy(
                ref.at[:, :, v * ez : (v + 1) * ez], stored.at[n, v], in_sem.at[n, v]
            )
            copy.start()
            arriving.append(copy)

    sub = lax.broadcasted_iota(jnp.int32, (subs, lanes), 0)
    row_y = lax.rem(sub, ey)
    first_x, last_x = sub < ey, sub >= (ex - 1) * ey
    first_y, last_y = row_y == 0, row_y == ey - 1

    def shifted(plane, shift):
        return pltpu.roll(plane, shift % subs, 0)

    def sum_x(ref, q, zs, ys):
        last = q - 1
        for z in zs:
            for y in ys:
                p, r = y * q + z, (last * q + y) * q + z
                lo, hi = ref[p], ref[r]
                ref[p] = jnp.where(first_x, lo, lo + shifted(hi, ey))
                ref[r] = jnp.where(last_x, hi, hi + shifted(lo, -ey))

    def sum_y(ref, q, zs):
        last = q - 1
        for z in zs:
            for x in range(q):
                p, r = x * q * q + z, (x * q + last) * q + z
                lo, hi = ref[p], ref[r]
                ref[p] = jnp.where(first_y, lo, lo + shifted(hi, 1))
                ref[r] = jnp.where(last_y, hi, hi + shifted(lo, -1))

    def local_sum(ref, q, zs):
        sum_x(ref, q, zs, range(q))
        sum_y(ref, q, zs)

    def edge(dx, dy, q):
        xs = range(q) if dx == 0 else [0 if dx < 0 else q - 1]
        ys = range(q) if dy == 0 else [0 if dy < 0 else q - 1]
        planes = [(x * q + y) * q + z for x in xs for y in ys for z in range(q - 1)]
        e, f = (0 if dx < 0 else ex - 1), (0 if dy < 0 else ey - 1)
        if dy == 0:
            return planes, ey, slice(e * ey, (e + 1) * ey)
        if dx == 0:
            return planes, ex, pl.ds(f, ex, stride=ey)
        return planes, 1, slice(e * ey + f, e * ey + f + 1)

    def whole_rows(count):
        return -(-count // tile) * tile

    pending = []

    def start_exchange(level, stage, fields, ways=range(len(DIRS))):
        send, recv, sems = level
        copies = []
        for d in ways:
            dx, dy = DIRS[d]
            at = 0
            for ref, q in fields:
                planes, count, rows = edge(dx, dy, q)
                for p in planes:
                    send[stage, d, at : at + count, :] = ref[p, rows, :]
                    at += count
            total = whole_rows(at)
            copy = pltpu.make_async_remote_copy(
                src_ref=send.at[stage, d, pl.ds(0, total)],
                dst_ref=recv.at[stage, d, pl.ds(0, total)],
                send_sem=sems.at[0, stage, d],
                recv_sem=sems.at[1, stage, d],
                device_id=target(dx, dy),
                device_id_type=MESH,
            )
            copy.start()
            copies.append(copy)
        return copies

    def finish_exchange(level, stage, fields, copies, finals, meanwhile=None):
        _, recv, _ = level
        for d in reversed(range(len(DIRS))):
            dx, dy = DIRS[d]
            copies[d].wait_recv()
            at = 0
            for ref, q in fields:
                planes, count, rows = edge(-dx, -dy, q)
                for p in planes:
                    ref[p, rows, :] = ref[p, rows, :] + recv[stage, d, at : at + count, :]
                    at += count
            if d == len(DIRS) - 2:
                for (ref, q), final in zip(fields, finals):
                    boundary(ref, ref, q, final, range(1, q - 1))
                if meanwhile is not None:
                    meanwhile()
        pending.extend(copies)
        for (ref, q), final in zip(fields, finals):
            boundary(ref, ref, q, final, (0, q - 1))

    def boundary(ref, dst, q, final, ys):
        for x in range(q):
            for y in ys:
                if x in (0, q - 1) or y in (0, q - 1):
                    p = (x * q + y) * q
                    for z in range(q - 1):
                        value = final(p + z, ref[p + z])
                        dst[p + z] = value
                        if z == 0:
                            dst[p + q - 1] = pltpu.roll(value, lanes - 1, 1)

    def interior(ref, q, final, dst=None):
        dst = ref if dst is None else dst
        for x in range(1, q - 1):
            for y in range(1, q - 1):
                for z in range(q):
                    p = (x * q + y) * q + z
                    dst[p] = final(p, ref[p])

    fine = (fine_send, fine_recv, fine_sems)
    rough = (coarse_send, coarse_recv, coarse_sems)

    def start_line(which, along_x, first, second):
        out, slots, sems = (
            (line_x_send, line_x, line_x_sem) if along_x else (line_y_send, line_y, line_y_sem)
        )
        count = nx if along_x else ny
        out[which, 0:1] = first
        out[which, 1:2] = second
        copies = []
        for o in range(1, count):
            copy = pltpu.make_async_remote_copy(
                src_ref=out.at[which],
                dst_ref=slots.at[which, o],
                send_sem=line_send_sem.at[which, 0 if along_x else 1, o],
                recv_sem=sems.at[which, o],
                device_id=target(o, 0) if along_x else target(0, o),
                device_id_type=MESH,
            )
            copy.start()
            copies.append(copy)
        return copies

    def finish_line(which, along_x, copies):
        out, slots = (line_x_send, line_x) if along_x else (line_y_send, line_y)
        count = nx if along_x else ny
        for copy in copies:
            copy.wait_recv()
        pending.extend(copies)
        total = out[which]
        for o in range(1, count):
            total = total + slots[which, o]
        return total[0:1], total[1:2]

    def inverse_estimate(first, second):
        first = jnp.sum(first, axis=1, keepdims=True)
        second = jnp.sum(second, axis=1, keepdims=True)
        return 1.0 / jnp.sqrt(second / (first + 1e-06))

    def coefficients(inv_est):
        power = inv_est
        out = []
        for c in CHEB:
            out.append(jnp.broadcast_to(c * power, (subs, lanes)))
            power = power * inv_est
        return out

    net = Lanes(QF, tile, ez)
    group = tile // ey

    def permuted(plane, index):
        tiles = [
            jnp.take_along_axis(plane[h * tile : (h + 1) * tile], index, axis=1)
            for h in range(subs // tile)
        ]
        return jnp.concatenate(tiles, axis=0)

    def read_planes(n, dst):
        for x in range(QF):
            for y in range(QF):
                for h in range(subs // tile):
                    blocks = []
                    for v in range(QF):
                        parts = [
                            stored[n, v, (h * group + e) * QF + x, pl.ds(y, ey, stride=QF), :]
                            for e in range(group)
                        ]
                        blocks.append(jnp.concatenate(parts, axis=0))
                    for z, block in enumerate(net.mix(blocks)):
                        dst[(x * QF + y) * QF + z, h * tile : (h + 1) * tile, :] = block

    (
        cflux,
        cmass,
        cinv,
        rload,
        cpow,
        cpow_2,
        rw0,
        rw1,
        rw2,
        crhs,
        cw0,
        cw1,
        ccor,
    ) = [coarse.at[i] for i in range(13)]

    for copy in arriving[:QF]:
        copy.wait()
    read_planes(0, load)
    for z in range(QF):
        for x in range(QF):
            for y in range(QF):
                p = (x * QF + y) * QF + z
                load[p] = float(FINE_W[x] * FINE_W[y] * FINE_W[z]) * permuted(load[p], net.pick[z])
    for a in range(QF * QF):
        line = z_sum([load[a * QF], load[a * QF + QF - 1]], lanes)
        load[a * QF] = line[0]
        load[a * QF + QF - 1] = line[1]
    local_sum(load, QF, range(QF - 1))

    def each(q, body):
        @pl.loop(0, q * q)
        def _(a):
            for i in range(q):
                body(a * q + i)

    def squares(q, values):
        def body(a, acc):
            for i in range(q):
                v = values(a * q + i)
                acc = acc + v * v
            return acc

        total = lax.fori_loop(0, q * q, body, jnp.zeros((subs, lanes), jnp.float32))
        return jnp.sum(total, axis=0, keepdims=True)

    def store(dst, values):
        def body(p):
            dst[p] = values(p)

        return body

    def half_unless(mask):
        return jnp.where(mask, 1.0, 0.5)

    def weighted(line, ends):
        if ends is None:
            return line
        return [half_unless(ends[0]) * line[0]] + line[1:-1] + [half_unless(ends[1]) * line[-1]]

    def restrict(field, dst, summed):
        ends_x = (first_x, last_x) if summed else None
        ends_y = (first_y, last_y) if summed else None

        for a in range(QF):
            for c in range(QF):
                line = [field[i * QF * QF + a * QF + c] for i in range(QF)]
                line = dense(TRANSFER, weighted(line, ends_x))
                for i in range(QC):
                    tmp_a[i * QF * QF + a * QF + c] = line[i]

        for a in range(QC):
            for c in range(QF):
                line = [tmp_a[a * QF * QF + i * QF + c] for i in range(QF)]
                line = dense(TRANSFER, weighted(line, ends_y))
                for i in range(QC):
                    tmp_b[a * QC * QF + i * QF + c] = line[i]

        for a in range(QC):
            for c in range(QC):
                line = dense(RESTRICT, [tmp_b[a * QC * QF + c * QF + i] for i in range(QF)])
                line = z_sum(line, lanes)
                for i in range(QC):
                    dst[a * QC * QC + c * QC + i] = line[i]

    def scaled_fluxes(flux, scaled, table):
        q = table.shape[0]
        square = 1.0 / row_scales(table) ** 2

        for x in range(q):
            for y in range(q):
                for z in range(q):
                    p = (x * q + y) * q + z
                    value = flux[p]
                    for axis, i in enumerate((x, y, z)):
                        scaled[axis, p] = float(square[i]) * value

    def start_apply(src, dst):
        return lambda: operator_start(src, dst, fluxes, mass, FINE_D, lanes)

    def apply_and_send(src, dst, stage, started=True):
        copies = []

        def first_part():
            sum_x(dst, QF, inner_f, (0, QF - 1))
            copies.extend(start_exchange(fine, stage, [(dst, QF)], range(6)))

        local_op(src, dst, fluxes, mass, FINE_D, lanes, first_part, started)
        sum_x(dst, QF, inner_f, range(1, QF - 1))
        sum_y(dst, QF, inner_f)
        return copies + start_exchange(fine, stage, [(dst, QF)], range(6, len(DIRS)))

    def apply_coarse(src, dst):
        local_op(src, dst, cfluxes, cmass, COARSE_D, lanes)

    def apply_coarse_and_send(src, dst, stage):
        copies = []

        def first_part():
            sum_x(dst, QC, inner_c, (0, QC - 1))
            copies.extend(start_exchange(rough, stage, [(dst, QC)], range(6)))

        local_op(src, dst, cfluxes, cmass, COARSE_D, lanes, first_part)
        sum_x(dst, QC, inner_c, range(1, QC - 1))
        sum_y(dst, QC, inner_c)
        return copies + start_exchange(rough, stage, [(dst, QC)], range(6, len(DIRS)))

    keep = lambda p, v: v
    invert = lambda p, v: 1.0 / v
    scaled = lambda p, v: inv[p] * v
    cscaled = lambda p, v: cinv[p] * v
    inner_f, inner_c = range(QF - 1), range(QC - 1)

    pl.semaphore_wait(barrier, len(greeted))
    f_load = start_exchange(fine, 0, [(load, QF)])

    pick = {0: 0, 2: 1, 4: 2}
    for n, full, part in ((1, flux, cflux), (2, mass, cmass)):
        for copy in arriving[n * QF : (n + 1) * QF]:
            copy.wait()
        read_planes(n, full)
        for z in range(QF):
            for x in range(QF):
                for y in range(QF):
                    p = (x * QF + y) * QF + z
                    value = permuted(full[p], net.pick[z])
                    full[p] = float(FINE_W[x] * FINE_W[y] * FINE_W[z]) * value
                    if x in pick and y in pick and z in pick:
                        i, j, k = pick[x], pick[y], pick[z]
                        weight = float(COARSE_W[i] * COARSE_W[j] * COARSE_W[k])
                        part[(i * QC + j) * QC + k] = weight * value

    local_diag(inv, flux, mass, FINE_D, lanes)
    local_sum(inv, QF, inner_f)
    f_diag = start_exchange(fine, 1, [(inv, QF)])

    local_sum(load, QF, [QF - 1])
    restrict(load, rload, True)
    local_sum(rload, QC, inner_c)
    local_diag(cinv, cflux, cmass, COARSE_D, lanes)
    local_sum(cinv, QC, inner_c)
    c_0 = start_exchange(rough, 0, [(cinv, QC), (rload, QC)])
    scaled_fluxes(flux, fluxes, FINE_D)
    scaled_fluxes(cflux, cfluxes, COARSE_D)
    interior(inv, QF, invert)

    finish_exchange(fine, 0, [(load, QF)], f_load, [keep], start_apply(load, power))
    f_power = apply_and_send(load, power, 2)
    interior(power, QF, scaled)

    interior(load, QF, scaled, b0)

    def start_b0():
        boundary(load, b0, QF, scaled, range(1, QF - 1))
        operator_start(b0, b1, fluxes, mass, FINE_D, lanes)

    finish_exchange(fine, 1, [(inv, QF)], f_diag, [invert], start_b0)
    boundary(load, b0, QF, scaled, (0, QF - 1))
    f_w0 = apply_and_send(b0, b1, 3)

    local_sum(b1, QF, [QF - 1])
    restrict(b1, rw0, True)
    local_sum(rw0, QC, inner_c)
    interior(b1, QF, scaled)
    interior(cinv, QC, invert)
    finish_exchange(rough, 0, [(cinv, QC), (rload, QC)], c_0, [invert, keep])
    apply_coarse(rload, cpow)
    local_sum(cpow, QC, inner_c)
    c_1 = start_exchange(rough, 1, [(cpow, QC), (rw0, QC)])
    interior(cpow, QC, cscaled)

    finish_exchange(fine, 2, [(power, QF)], f_power, [scaled], start_apply(power, power_2))
    f_power_2 = apply_and_send(power, power_2, 4)
    interior(power_2, QF, scaled)

    finish_exchange(fine, 3, [(b1, QF)], f_w0, [scaled], start_apply(b1, b2))
    f_w1 = apply_and_send(b1, b2, 5)

    local_sum(b2, QF, [QF - 1])
    restrict(b2, rw1, True)
    local_sum(rw1, QC, inner_c)
    interior(b2, QF, scaled)
    finish_exchange(rough, 1, [(cpow, QC), (rw0, QC)], c_1, [cscaled, keep])
    apply_coarse(cpow, cpow_2)
    local_sum(cpow_2, QC, inner_c)
    c_2 = start_exchange(rough, 2, [(cpow_2, QC), (rw1, QC)])
    interior(cpow_2, QC, cscaled)
    sum_first = squares(QF, lambda p: power[p])

    finish_exchange(fine, 4, [(power_2, QF)], f_power_2, [scaled])
    sum_second = squares(QF, lambda p: power_2[p])
    line = start_line(0, True, sum_first, sum_second)

    finish_exchange(fine, 5, [(b2, QF)], f_w1, [scaled], start_apply(b2, power))
    across = []

    def forward():
        across.extend(start_line(0, False, *finish_line(0, True, line)))

    local_op(b2, power, fluxes, mass, FINE_D, lanes, forward, True)
    restrict(power, rw2, False)
    local_sum(rw2, QC, inner_c)
    c_3 = start_exchange(rough, 3, [(rw2, QC)])

    finish_exchange(rough, 2, [(cpow_2, QC), (rw1, QC)], c_2, [cscaled, keep])
    csum_first = squares(QC, lambda p: cpow[p])
    csum_second = squares(QC, lambda p: cpow_2[p])
    cline = start_line(1, True, csum_first, csum_second)
    scale = coefficients(inverse_estimate(*finish_line(0, False, across)))
    each(
        QF,
        store(smooth, lambda p: scale[0] * b0[p] + scale[1] * b1[p] + scale[2] * b2[p]),
    )
    each(QC, store(crhs, lambda p: rload[p] - (scale[0] * rw0[p] + scale[1] * rw1[p])))

    first = lambda p, v: cinv[p] * (crhs[p] - scale[2] * v)
    interior(rw2, QC, first)
    finish_exchange(rough, 3, [(rw2, QC)], c_3, [first])
    c_4 = apply_coarse_and_send(rw2, cw0, 4)
    interior(cw0, QC, cscaled)
    cline = start_line(1, False, *finish_line(1, True, cline))

    finish_exchange(rough, 4, [(cw0, QC)], c_4, [cscaled])
    c_5 = apply_coarse_and_send(cw0, cw1, 5)
    interior(cw1, QC, cscaled)
    cscale = coefficients(inverse_estimate(*finish_line(1, False, cline)))
    each(QC, store(ccor, lambda p: cscale[0] * rw2[p] + cscale[1] * cw0[p]))

    for copy in pending:
        copy.wait_send()
    pending.clear()

    finish_exchange(rough, 5, [(cw1, QC)], c_5, [cscaled])
    each(QC, store(ccor, lambda p: ccor[p] + cscale[2] * cw1[p]))

    def write_planes(dst, planes, q, lane_net):
        for x in range(q):
            for y in range(q):
                for h in range(subs // tile):
                    rows = slice(h * tile, (h + 1) * tile)
                    placed = [planes[(x * q + y) * q + z, rows, :] for z in range(q)]
                    for v, block in enumerate(lane_net.unmix(placed)):
                        for e in range(group):
                            part = block[e * ey : (e + 1) * ey]
                            dst[v, (h * group + e) * q + x, pl.ds(y, ey, stride=q), :] = part

    cnet = Lanes(QC, tile, ez)
    for z in range(QC):
        for a in range(QC * QC):
            tmp_b[a * QC + z] = permuted(ccor[a * QC + z], cnet.place[z])
    write_planes(cresult, tmp_b, QC, cnet)
    for y in range(QC):
        for z in range(QC):
            line = dense(INTERP, [ccor[i * QC * QC + y * QC + z] for i in range(QC)])
            for i in range(QF):
                tmp_a[(i * QC + y) * QC + z] = line[i]
    for x in range(QF):
        for z in range(QC):
            line = dense(INTERP, [tmp_a[(x * QC + i) * QC + z] for i in range(QC)])
            for i in range(QF):
                tmp_b[(x * QF + i) * QC + z] = line[i]
    for z in range(QF):
        for a in range(QF * QF):
            p = a * QF + z
            lifted = dense(INTERP[z : z + 1], [tmp_b[a * QC + i] for i in range(QC)])[0]
            smooth[p] = permuted(smooth[p] + lifted, net.place[z])
    write_planes(result, smooth, QF, net)
    for copy in pending:
        copy.wait_send()


def hand_over(result, cresult, out_hbm, cor_hbm, out_sem, cor_sem):
    copies = []
    for blocks, whole, sems in ((result, out_hbm, out_sem), (cresult, cor_hbm, cor_sem)):
        count, _, _, ez = blocks.shape
        for v in range(count):
            lanes = whole.at[:, :, v * ez : (v + 1) * ez]
            copies.append(pltpu.make_async_copy(blocks.at[v], lanes, sems.at[v]))
    for copy in copies:
        copy.start()
    for copy in copies:
        copy.wait()


def on_device(nx, ny, source, conductivity, absorption):
    px, py, pz = source.shape
    ex, ey, ez = px // QF, py // QF, pz // QF
    subs = ex * ey
    face = max(ex, ey)
    f32 = jnp.float32
    dirs = len(DIRS)
    longest = max(nx, ny)
    fine_rows = -(-QF * (QF - 1) * face // 8) * 8
    coarse_rows = -(-2 * QC * (QC - 1) * face // 8) * 8
    scratch = [
        pltpu.VMEM((3, QF, px, py, ez), f32),
        *[pltpu.VMEM((QF**3, subs, ez), f32)] * 8,
        pltpu.VMEM((3, QF**3, subs, ez), f32),
        pltpu.VMEM((3, QC**3, subs, ez), f32),
        *[pltpu.VMEM((QF**3, subs, ez), f32)] * 2,
        pltpu.VMEM((13, QC**3, subs, ez), f32),
        pltpu.VMEM((QF * QF * QC, subs, ez), f32),
        pltpu.VMEM((QF * QF * QC, subs, ez), f32),
        *[pltpu.VMEM((FINE_STAGES, dirs, fine_rows, ez), f32)] * 2,
        *[pltpu.VMEM((COARSE_STAGES, dirs, coarse_rows, ez), f32)] * 2,
        pltpu.VMEM((2, 8, ez), f32),
        pltpu.VMEM((2, nx, 8, ez), f32),
        pltpu.VMEM((2, 8, ez), f32),
        pltpu.VMEM((2, ny, 8, ez), f32),
        pltpu.SemaphoreType.DMA((3, QF)),
        pltpu.SemaphoreType.DMA((2, FINE_STAGES, dirs)),
        pltpu.SemaphoreType.DMA((2, COARSE_STAGES, dirs)),
        pltpu.SemaphoreType.DMA((2, 2, longest)),
        pltpu.SemaphoreType.DMA((2, nx)),
        pltpu.SemaphoreType.DMA((2, ny)),
    ]
    anywhere = pl.BlockSpec(memory_space=pl.ANY)
    out, cor = pl.pallas_call(
        functools.partial(kernel, nx, ny),
        out_shape=(
            jax.ShapeDtypeStruct((QF, px, py, ez), f32),
            jax.ShapeDtypeStruct((QC, ex * QC, ey * QC, ez), f32),
        ),
        in_specs=[pl.BlockSpec(memory_space=pltpu.HBM)] * 3,
        out_specs=(pl.BlockSpec(memory_space=pltpu.VMEM),) * 2,
        scratch_shapes=scratch,
        compiler_params=pltpu.CompilerParams(
            collective_id=0, has_side_effects=True, vmem_limit_bytes=52 * 1024 * 1024
        ),
    )(source, conductivity, absorption)
    return pl.pallas_call(
        hand_over,
        out_shape=(
            jax.ShapeDtypeStruct(source.shape, f32),
            jax.ShapeDtypeStruct((ex * QC, ey * QC, ez * QC), f32),
        ),
        in_specs=[anywhere] * 2,
        out_specs=(pl.BlockSpec(memory_space=pltpu.HBM),) * 2,
        scratch_shapes=[pltpu.SemaphoreType.DMA((QF,)), pltpu.SemaphoreType.DMA((QC,))],
        compiler_params=pltpu.CompilerParams(vmem_limit_bytes=1024 * 1024),
    )(out, cor)


def solution(mesh):
    spec = P("gx", "gy", None)
    return jax.shard_map(
        functools.partial(on_device, mesh.shape["gx"], mesh.shape["gy"]),
        mesh=mesh,
        in_specs=(spec,) * 3,
        out_specs=(spec, spec),
        check_vma=False,
    )
```
